128 devices in a mesh: row: 8 (over y_hi, z), col: 16 (over y_lo, x, core).
Axes of the slice: x: 4, y: 4 (y_hi: 2, y_lo: 2; y = y_hi * 2 + y_lo), z: 4, core: 2. Of those that a mesh axis runs over, the one named last changes fastest.
Arguments:
- build_key: int32 [16, 16, 128], P('col', 'row'), may hold values from -1 to 63, as said below
- build_part: int32 [16, 16], P('col', 'row'), may hold values from 0 to 1023, as said below
- build_payload: float32 [16, 16, 128, 128], P('col', 'row'), may hold values from -6 to 6
- probe_key: int32 [8, 16, 16, 8, 128], P('row', 'col'), may hold values from -2 to 63, as said below
- probe_part: int32 [8, 16, 16, 8, 128], P('row', 'col'), may hold values from 0 to 1023, as said below
Outputs:
- joined: float32 [8, 16, 16, 8, 128, 128], P('row', 'col')
- match_position: float32 [8, 16, 16, 8, 128], P('row', 'col')
- match_rate: float32 [1024], replicated
The draws below stay inside these ranges and needn't reach their ends.
Inputs may be any that keep to these rules, and one draw needn't show every extreme that they name: Each column c owns a set of 64 partitions, disjoint from the other columns' sets; build_part[c, t] lies in column c's set. `build_key`: -1 marks padding rows, which lie at the end of a tile. `probe_key`: -2 marks padding rows, which lie at the end of a tile. probe_part[r, s, c, q, i] lies in the set of partitions owned by column c.
All inputs are finite; a program needn't handle non-finite values.
Results may differ from the reference program's by a relative error of at most 0.0003.
Values sent between devices are 32-bit elements; how exact they have to be, the bound alone decides.
A program may use at most 256 MiB of HBM per device.

```python
import jax
import jax.numpy as jnp
from jax import lax

PARTS_SIZE = 1024
TILE = 128
PAYLOAD = 128
KEY_RANGE = 64
PROBE_TILES = 8
COLUMN_TILES = 16
N_ROW = 8
N_COL = 16


def owned_table(key):
    shuffled = jax.random.permutation(jax.random.fold_in(key, 7), PARTS_SIZE)
    return shuffled.reshape(N_COL, PARTS_SIZE // N_COL).astype(jnp.int32)


def skewed_pick(key, dims):
    share = PARTS_SIZE // N_COL
    picked = jax.random.randint(key, dims, 0, share)
    return picked * picked // share


def draw_build_part(key, part):
    table = owned_table(key)
    picks = skewed_pick(jax.random.fold_in(key, 1), (N_COL, COLUMN_TILES))
    owners = jnp.arange(N_COL)[:, None]
    return table[owners, picks].astype(jnp.int32)


def draw_build_key(key, part):
    base = jax.random.randint(jax.random.fold_in(key, 2), (N_COL, COLUMN_TILES, TILE), 0, KEY_RANGE)
    filled = jax.random.randint(jax.random.fold_in(key, 3), (N_COL, COLUMN_TILES, 1), TILE // 4, TILE + 1)
    places = jnp.arange(TILE)[None, None, :]
    return jnp.where(places < filled, base, -1).astype(jnp.int32)


def draw_probe_part(key, part):
    table = owned_table(key)
    picks = skewed_pick(jax.random.fold_in(key, 4), (N_ROW, N_COL, N_COL, PROBE_TILES, TILE))
    owners = jnp.arange(N_COL)[None, None, :, None, None]
    return table[owners, picks].astype(jnp.int32)


def draw_probe_key(key, part):
    base = jax.random.randint(jax.random.fold_in(key, 5), (N_ROW, N_COL, N_COL, PROBE_TILES, TILE), 0, KEY_RANGE)
    filled = jax.random.randint(jax.random.fold_in(key, 6), (N_ROW, N_COL, N_COL, PROBE_TILES, 1), TILE // 4, TILE + 1)
    places = jnp.arange(TILE)[None, None, None, None, :]
    return jnp.where(places < filled, base, -2).astype(jnp.int32)


def shard_levels(stream_key, shape, split, low, largest):
    level, own = 1.0, jax.random.fold_in(stream_key, 6)
    for axis_at, blocks in split:
        draws = jnp.exp(jax.random.uniform(jax.random.fold_in(own, axis_at), (blocks,), jnp.float32, low / len(split), largest / len(split)))
        level = level * jnp.repeat(draws, shape[axis_at] // blocks).reshape([-1 if axis == axis_at else 1 for axis in range(len(shape))])
    return level


def centred(stream_key, shape, width, bound, cuts=(), held_as=jnp.bfloat16):
    values = width * jax.random.normal(stream_key, shape, jnp.float32)
    if cuts:
        values = values * shard_levels(stream_key, shape, cuts, -0.22, 0.18)
    return jnp.clip(values, -bound, bound).astype(held_as)


def setup_inputs(seed: int = 0) -> dict:
    arg_keys = jax.random.split(jax.random.key(seed), 6)
    build_key = draw_build_key(jax.random.fold_in(arg_keys[5], 71), 0)
    build_part = draw_build_part(jax.random.fold_in(arg_keys[5], 71), 0)
    build_payload = centred(arg_keys[2], (N_COL, COLUMN_TILES, TILE, PAYLOAD), 1.0, 6.0, ((0, 16), (1, 8)), jnp.float32)
    probe_key = draw_probe_key(jax.random.fold_in(arg_keys[5], 71), 0)
    probe_part = draw_probe_part(jax.random.fold_in(arg_keys[5], 71), 0)
    return dict(build_key=build_key, build_part=build_part, build_payload=build_payload, probe_key=probe_key, probe_part=probe_part)


def tile_join(probe_keys, probe_parts, build_keys, build_parts, payload, positions):
    count_tiles = build_keys.shape[0]
    tile_rows = build_keys.shape[1]
    flat_keys = build_keys.reshape(-1)
    flat_parts = jnp.broadcast_to(build_parts.reshape(-1, 1), (count_tiles, tile_rows)).reshape(-1)
    flat_payload = payload.reshape(count_tiles * tile_rows, payload.shape[-1])

    def one_block(block_args):
        block_keys, block_parts = block_args
        matched = ((block_keys[:, None] == flat_keys[None, :]) & (block_parts[:, None] == flat_parts[None, :])).astype(jnp.float32)
        summed = jnp.dot(matched, flat_payload, precision=lax.Precision.HIGHEST, preferred_element_type=jnp.float32)
        placed = jnp.dot(matched, positions, precision=lax.Precision.HIGHEST, preferred_element_type=jnp.float32)
        return summed, placed, jnp.sum(matched, axis=1)

    return lax.map(one_block, (probe_keys, probe_parts))


def reference(build_key, build_part, build_payload, probe_key, probe_part):
    positions = jnp.arange(COLUMN_TILES * TILE, dtype=jnp.int32).astype(jnp.float32) / float(COLUMN_TILES * TILE)

    def owner_block(index):
        row_index = index // N_COL
        col_index = index % N_COL
        keys_here = lax.dynamic_index_in_dim(probe_key, row_index, 0, keepdims=False)
        keys_here = lax.dynamic_index_in_dim(keys_here, col_index, 1, keepdims=False)
        parts_here = lax.dynamic_index_in_dim(probe_part, row_index, 0, keepdims=False)
        parts_here = lax.dynamic_index_in_dim(parts_here, col_index, 1, keepdims=False)
        build_keys = lax.dynamic_index_in_dim(build_key, col_index, 0, keepdims=False)
        build_parts = lax.dynamic_index_in_dim(build_part, col_index, 0, keepdims=False)
        payload = lax.dynamic_index_in_dim(build_payload, col_index, 0, keepdims=False)
        return tile_join(keys_here.reshape(N_COL, PROBE_TILES * TILE), parts_here.reshape(N_COL, PROBE_TILES * TILE), build_keys, build_parts, payload, positions)

    joined, placed, counts = lax.map(owner_block, jnp.arange(N_ROW * N_COL, dtype=jnp.int32))
    joined = joined.reshape(N_ROW, N_COL, N_COL, PROBE_TILES, TILE, PAYLOAD).transpose(0, 2, 1, 3, 4, 5)
    placed = placed.reshape(N_ROW, N_COL, N_COL, PROBE_TILES, TILE).transpose(0, 2, 1, 3, 4)
    counts = counts.reshape(N_ROW, N_COL, N_COL, PROBE_TILES, TILE).transpose(0, 2, 1, 3, 4)
    part_ids = probe_part.reshape(-1)
    match_total = jax.ops.segment_sum(counts.reshape(-1), part_ids, num_segments=PARTS_SIZE)
    live_rows = (probe_key >= 0).astype(jnp.float32).reshape(-1)
    live_total = jax.ops.segment_sum(live_rows, part_ids, num_segments=PARTS_SIZE)
    return joined, placed, match_total / jnp.maximum(live_total, 1.0)
```

```python
import functools

import jax
import jax.numpy as jnp
from jax import lax
from jax.experimental import pallas as pl
from jax.experimental.pallas import tpu as pltpu
from jax.sharding import Mesh
from jax.sharding import PartitionSpec as P

PARTS_SIZE = 1024
KEYS = 64
ROW = ("row_0", "row_1")
COL = ("col_0", "col_1", "col_2")
ALL = ROW + COL
MESH = pl.DeviceIdType.MESH

PIECE = 136
CUTS = ((0, 48), (48, 48), (96, 40))
ORDERS = ((0, 1, 2), (1, 2, 0), (2, 0, 1))


def table_of(tile_base, key_ref, part_ref, payload_ref):
    lane = lax.broadcasted_iota(jnp.int32, (8, 128), 1)
    sub = lax.broadcasted_iota(jnp.int32, (8, 128), 0)
    keys_col = lax.broadcasted_iota(jnp.int32, (KEYS, 128), 0)
    side_lhs = jnp.where(sub == 0, lane.astype(jnp.float32) / 2048.0, jnp.where(sub == 1, 1.0, 0.0))
    sums, sides = [], []
    for t in range(2):
        onehot = (keys_col == key_ref[0, t : t + 1, :]).astype(jnp.float32)
        sums.append(
            jnp.dot(onehot, payload_ref[0, t], precision=lax.Precision.HIGHEST, preferred_element_type=jnp.float32)
        )
        side = lax.dot_general(
            side_lhs, onehot, (((1,), (1,)), ((), ())), preferred_element_type=jnp.float32
        )
        start = (tile_base + t).astype(jnp.float32) / 16.0
        sides.append(side + jnp.where(sub[:, :KEYS] == 0, start * side[1:2, :], 0.0))
    table = jnp.concatenate(sums, axis=0).T
    side = jnp.concatenate(sides, axis=1)
    for t in range(2):
        side = jnp.where(sub == 2 + t, part_ref[0, t].astype(jnp.float32), side)
    return table, side


def gather_kernel(key_ref, part_ref, payload_ref, g_ref, recv, pair_recv, send):
    yh, z, yl, x, core = (lax.axis_index(a) for a in ALL)
    here = (x, yh * 2 + yl, z)

    def device(at, k):
        return (at[1] // 2, at[2], at[1] % 2, at[0], k)

    def slot(at, k):
        return (((at[1] % 2) * 4 + at[0]) * 2 + k) * 8 + (at[1] // 2) * 4 + at[2]

    def shifted(at, dim, delta):
        return tuple((v + delta) % 4 if d == dim else v for d, v in enumerate(at))

    def place(p, off):
        order = ORDERS[p]
        at = list(here)
        for level in range(3):
            at[order[level]] = (at[order[level]] + off[level]) % 4
        return slot(tuple(at), core)

    def block(p, index):
        return g_ref.at[index, pl.ds(CUTS[p][0], CUTS[p][1])]

    def push(p, off, level, delta):
        far = tuple((o - delta + 4) % 4 if n == level else o for n, o in enumerate(off))
        ref = block(p, place(p, off))
        pltpu.make_async_remote_copy(
            src_ref=ref, dst_ref=ref, send_sem=send.at[p], recv_sem=recv.at[p, far[0] * 16 + far[1] * 4 + far[2]],
            device_id=device(shifted(here, ORDERS[p][level], delta + 4), core), device_id_type=MESH,
        ).start()

    def pair(p, off):
        ref = block(p, place(p, off))
        pltpu.make_async_remote_copy(
            src_ref=ref, dst_ref=ref, send_sem=send.at[p], recv_sem=pair_recv.at[p],
            device_id=device(here, 1 - core), device_id_type=MESH,
        ).start()

    def arrive(p, off):
        ref = block(p, place(p, off))
        pltpu.make_async_remote_copy(
            src_ref=ref, dst_ref=ref, send_sem=send.at[p], recv_sem=recv.at[p, off[0] * 16 + off[1] * 4 + off[2]],
            device_id=device(here, 1 - core), device_id_type=MESH,
        ).wait_recv()

    barrier = pltpu.get_barrier_semaphore()
    for dim in range(3):
        for delta in (1, 3):
            pl.semaphore_signal(barrier, inc=1, device_id=device(shifted(here, dim, delta), core), device_id_type=MESH)
    pl.semaphore_signal(barrier, inc=1, device_id=device(here, 1 - core), device_id_type=MESH)

    table, side = table_of((yh * 4 + z) * 2, key_ref, part_ref, payload_ref)
    own = slot(here, core)
    g_ref[own, :128, :] = table
    g_ref[own, 128:, :] = side
    pl.semaphore_wait(barrier, 7)

    def both(p, off, level):
        push(p, off, level, 1)
        push(p, off, level, -1)

    for level in range(3):
        for p in range(3):
            both(p, (0, 0, 0), level)
    for p in range(3):
        pair(p, (0, 0, 0))
    for p in range(3):
        arrive(p, (3, 0, 0))
        push(p, (3, 0, 0), 0, 1)
    for level in (1, 2):
        for p in range(3):
            both(p, (3, 0, 0), level)
    for p in range(3):
        arrive(p, (1, 0, 0))
        both(p, (1, 0, 0), 1)
        both(p, (1, 0, 0), 2)
    for p in range(3):
        arrive(p, (2, 0, 0))
        both(p, (2, 0, 0), 1)
        both(p, (2, 0, 0), 2)
    for p in range(3):
        for o in (3, 1, 2):
            pair(p, (o, 0, 0))

    def turn(i):
        return i + (i // 2) * (5 - 2 * i)

    def second(i, carry):
        da = turn(i)
        delta = 1 - 2 * (da % 2)
        for p in range(3):
            near = (4 - delta) % 4
            for o in (3, 1):
                arrive(p, (da, o, 0))
                both(p, (da, o, 0), 2)
            push(p, (da, near, 0), 1, delta)
            for o in (3, 1):
                pair(p, (da, o, 0))
        return carry

    def second_far(i, carry):
        da = turn(i)
        for p in range(3):
            arrive(p, (da, 2, 0))
            both(p, (da, 2, 0), 2)
            pair(p, (da, 2, 0))
        return carry

    def third(i, carry):
        da, db = turn(i % 4), turn(i // 4)
        delta = 1 - 2 * ((da + db) % 2)
        near = (4 - delta) % 4
        for p in range(3):
            for o in (3, 1):
                arrive(p, (da, db, o))
            push(p, (da, db, near), 2, delta)
            for o in (3, 1):
                pair(p, (da, db, o))
        return carry

    def third_far(i, carry):
        da, db = turn(i % 4), turn(i // 4)
        for p in range(3):
            arrive(p, (da, db, 2))
            pair(p, (da, db, 2))
        return carry

    lax.fori_loop(0, 4, second, 0)
    lax.fori_loop(0, 4, second_far, 0)
    lax.fori_loop(0, 16, third, 0)
    lax.fori_loop(0, 16, third_far, 0)
    for p in range(3):
        rows = pl.ds(CUTS[p][0], CUTS[p][1])
        landed = g_ref.at[pl.ds(0, 64), rows]
        pltpu.make_async_copy(landed, landed, pair_recv.at[p]).wait()
        sent = g_ref.at[pl.ds(0, 127), rows]
        pltpu.make_async_copy(sent, sent, send.at[p]).wait()


def gather_tables(build_key, build_part, build_payload):
    return pl.pallas_call(
        gather_kernel,
        out_shape=jax.ShapeDtypeStruct((128, PIECE, 128), jnp.float32),
        in_specs=[
            pl.BlockSpec(memory_space=pltpu.VMEM),
            pl.BlockSpec(memory_space=pltpu.SMEM),
            pl.BlockSpec(memory_space=pltpu.VMEM),
        ],
        out_specs=pl.BlockSpec(memory_space=pltpu.VMEM),
        scratch_shapes=[
            pltpu.SemaphoreType.DMA((3, 64)),
            pltpu.SemaphoreType.DMA((3,)),
            pltpu.SemaphoreType.DMA((3,)),
        ],
        compiler_params=pltpu.CompilerParams(
            collective_id=0, has_side_effects=True, vmem_limit_bytes=16 * 1024 * 1024
        ),
        name="gather_tables",
    )(build_key, build_part, build_payload)


def join_kernel(key_ref, part_ref, g_ref, joined_ref, place_ref, stat_ref, table, hot, same):
    @pl.when(pl.program_id(0) == 0)
    def _():
        stat_ref[...] = jnp.zeros_like(stat_ref)

    keys = key_ref[0]
    parts = part_ref[0]
    parts_f = parts.astype(jnp.float32)
    for r in range(8):
        piece = g_ref[r]
        high = piece.astype(jnp.bfloat16)
        low = (piece - high.astype(jnp.float32)).astype(jnp.bfloat16)
        lanes = pl.ds(r * 128, 128)
        table[0:128, lanes] = high[:128]
        table[128:256, lanes] = low[:128]
        table[256:272, lanes] = jnp.concatenate(
            [high[128:].astype(jnp.float32), low[128:].astype(jnp.float32)], axis=0
        ).astype(jnp.bfloat16)
        for t in range(2):
            same[r * 2 + t] = (parts_f == piece[130 + t : 131 + t, :]).astype(jnp.float32)
    key_col = lax.broadcasted_iota(jnp.int32, (KEYS, 128), 0)
    counts = []
    for q2 in range(4):
        for h in range(2):
            q = q2 * 2 + h
            key_hot = (key_col == keys[q : q + 1, :]).astype(jnp.float32).astype(jnp.bfloat16)
            lanes = pl.ds(h * 128, 128)
            for t in range(16):
                row = jnp.broadcast_to(same[t, q : q + 1, :], (16, 128)).astype(jnp.bfloat16)
                hot[q2, t * KEYS : (t + 1) * KEYS, lanes] = key_hot * jnp.concatenate([row] * 4, axis=0)
        out = jnp.dot(table[...], hot[q2], preferred_element_type=jnp.float32)
        sums = out[:128] + out[128:256]
        joined_ref[0, q2 * 2] = sums[:, :128].T
        joined_ref[0, q2 * 2 + 1] = sums[:, 128:].T
        side = out[256:264] + out[264:272]
        for h in range(2):
            place_ref[0, q2 * 2 + h : q2 * 2 + h + 1, :] = side[0:1, h * 128 : (h + 1) * 128]
            counts.append(side[1:2, h * 128 : (h + 1) * 128])

    count = jnp.concatenate(counts, axis=0)
    count_high = jnp.floor(count * (1.0 / 64.0))
    count_low = count - 64.0 * count_high
    live = (keys >= 0).astype(jnp.float32)
    major = parts // 128
    minor = parts - major * 128
    sub8 = lax.broadcasted_iota(jnp.int32, (8, 128), 0)
    sub128 = lax.broadcasted_iota(jnp.int32, (128, 128), 0)
    total = jnp.zeros((32, 128), jnp.float32)
    for q in range(8):
        major_hot = sub8 == major[q : q + 1, :]
        lhs = jnp.concatenate(
            [
                jnp.where(major_hot, v[q : q + 1, :], 0.0)
                for v in (count_high, count_low, live, jnp.zeros_like(live))
            ],
            axis=0,
        ).astype(jnp.bfloat16)
        rhs = (sub128 == minor[q : q + 1, :]).astype(jnp.float32).astype(jnp.bfloat16)
        total += lax.dot_general(lhs, rhs, (((1,), (1,)), ((), ())), preferred_element_type=jnp.float32)
    stat_ref[0:8, :] += 64.0 * total[0:8] + total[8:16]
    stat_ref[8:16, :] += total[16:24]


def join(probe_key, probe_part, tables):
    return pl.pallas_call(
        join_kernel,
        grid=(16,),
        out_shape=(
            jax.ShapeDtypeStruct((16, 8, 128, 128), jnp.float32),
            jax.ShapeDtypeStruct((16, 8, 128), jnp.float32),
            jax.ShapeDtypeStruct((16, 128), jnp.float32),
        ),
        in_specs=[
            pl.BlockSpec((1, 8, 128), lambda c: (c, 0, 0)),
            pl.BlockSpec((1, 8, 128), lambda c: (c, 0, 0)),
            pl.BlockSpec((8, PIECE, 128), lambda c: (c, 0, 0)),
        ],
        out_specs=(
            pl.BlockSpec((1, 8, 128, 128), lambda c: (c, 0, 0, 0)),
            pl.BlockSpec((1, 8, 128), lambda c: (c, 0, 0)),
            pl.BlockSpec((16, 128), lambda c: (0, 0)),
        ),
        scratch_shapes=[
            pltpu.VMEM((272, 1024), jnp.bfloat16),
            pltpu.VMEM((4, 1024, 256), jnp.bfloat16),
            pltpu.VMEM((16, 8, 128), jnp.float32),
        ],
        compiler_params=pltpu.CompilerParams(vmem_limit_bytes=32 * 1024 * 1024),
        name="join",
    )(probe_key, probe_part, tables)


def local(build_key, build_part, build_payload, probe_key, probe_part):
    tables = gather_tables(build_key, build_part, build_payload)
    joined, places, stats = join(probe_key.reshape(16, 8, 128), probe_part.reshape(16, 8, 128), tables)
    stats = lax.psum(stats, ALL)
    rate = stats[:8].reshape(PARTS_SIZE) / jnp.maximum(stats[8:].reshape(PARTS_SIZE), 1.0)
    return (joined[None, None], places[None, None], rate)


def solution(mesh):
    finer = Mesh(mesh.devices.reshape(2, 4, 2, 4, 2), ALL)
    return jax.shard_map(
        local,
        mesh=finer,
        in_specs=(
            P(COL, ROW, None),
            P(COL, ROW),
            P(COL, ROW, None, None),
            P(ROW, COL, None, None, None),
            P(ROW, COL, None, None, None),
        ),
        out_specs=(P(ROW, COL, None, None, None, None), P(ROW, COL, None, None, None), P()),
        check_vma=False,
    )
```

```python
import functools

import jax
import jax.numpy as jnp
from jax import lax
from jax.experimental import pallas as pl
from jax.experimental.pallas import tpu as pltpu
from jax.sharding import Mesh
from jax.sharding import PartitionSpec as P

PARTS_SIZE = 1024
KEYS = 64
ROW = ("row_0", "row_1")
COL = ("col_0", "col_1", "col_2")
ALL = ROW + COL
MESH = pl.DeviceIdType.MESH

PIECE = 136
CUTS = ((0, 48), (48, 48), (96, 40))
ORDERS = ((0, 1, 2), (1, 2, 0), (2, 0, 1))


def coded(part):
    major = part // 128
    return (128 + part - major * 128).astype(jnp.float32) * (1 << major).astype(jnp.float32)


def table_of(tile_base, key_ref, part_ref, payload_ref):
    lane = lax.broadcasted_iota(jnp.int32, (8, 128), 1)
    sub = lax.broadcasted_iota(jnp.int32, (8, 128), 0)
    keys_col = lax.broadcasted_iota(jnp.int32, (KEYS, 128), 0)
    side_lhs = jnp.where(sub == 0, lane.astype(jnp.float32) / 2048.0, jnp.where(sub == 1, 1.0, 0.0))
    sums, sides = [], []
    for t in range(2):
        onehot = (keys_col == key_ref[0, t : t + 1, :]).astype(jnp.float32)
        sums.append(
            jnp.dot(onehot, payload_ref[0, t], precision=lax.Precision.HIGHEST, preferred_element_type=jnp.float32)
        )
        side = lax.dot_general(
            side_lhs, onehot, (((1,), (1,)), ((), ())), preferred_element_type=jnp.float32
        )
        start = (tile_base + t).astype(jnp.float32) / 16.0
        sides.append(side + jnp.where(sub[:, :KEYS] == 0, start * side[1:2, :], 0.0))
    table = jnp.concatenate(sums, axis=0).T
    side = jnp.concatenate(sides, axis=1)
    for t in range(2):
        part = part_ref[0, t]
        side = jnp.where(sub == 2 + t, part.astype(jnp.float32), side)
        side = jnp.where(sub == 4 + t, coded(jnp.full((8, 128), part)), side)
    return table, side


def live_rows(key_ref, part_ref):
    sub8 = lax.broadcasted_iota(jnp.int32, (8, 128), 0)
    sub128 = lax.broadcasted_iota(jnp.int32, (128, 128), 0)

    def column(c, total):
        keys, parts = key_ref[c], part_ref[c]
        major = parts // 128
        minor = parts - major * 128
        lhs, rhs = [], []
        for q in range(8):
            live = (sub8 == major[q : q + 1, :]) & (keys[q : q + 1, :] >= 0)
            lhs.append(jnp.where(live, 1.0, 0.0))
            rhs.append((sub128 == minor[q : q + 1, :]).astype(jnp.float32).astype(jnp.bfloat16))
        lhs = jnp.concatenate(lhs, axis=1).astype(jnp.bfloat16)
        rhs = jnp.concatenate(rhs, axis=1)
        return total + lax.dot_general(lhs, rhs, (((1,), (1,)), ((), ())), preferred_element_type=jnp.float32)

    return lax.fori_loop(0, 16, column, jnp.zeros((8, 128), jnp.float32))


def match_rows(key_ref, part_ref, g_ref):
    sub8 = lax.broadcasted_iota(jnp.int32, (8, 128), 0)
    lane8 = lax.broadcasted_iota(jnp.int32, (8, 128), 1)
    label = (sub8 * 128 + lane8).astype(jnp.float32)
    first = lane8 < KEYS
    sub128 = lax.broadcasted_iota(jnp.int32, (128, 128), 0)
    key_at = jnp.where(sub128 >= KEYS, sub128 - KEYS, sub128)

    def column(c, total):
        keys, parts = key_ref[c], part_ref[c].astype(jnp.float32)
        pieces = pl.ds(c * 8, 8)
        count, even, odd = g_ref[pieces, 129, :], g_ref[pieces, 130, :], g_ref[pieces, 131, :]
        lhs, rhs = [], []
        for q in range(8):
            row = parts[q : q + 1, :]
            lhs.append(jnp.concatenate([jnp.where(even == row, 1.0, 0.0), jnp.where(odd == row, 1.0, 0.0)], axis=0))
            rhs.append((key_at == keys[q : q + 1, :]).astype(jnp.float32).astype(jnp.bfloat16))
        lhs = jnp.concatenate(lhs, axis=1).astype(jnp.bfloat16)
        rhs = jnp.concatenate(rhs, axis=1)
        seen = lax.dot_general(lhs, rhs, (((1,), (1,)), ((), ())), preferred_element_type=jnp.float32)
        pairs = jnp.where(first, seen[:8], seen[8:]) * count
        left = jnp.sum(jnp.where(first, pairs, 0.0), axis=1, keepdims=True)
        right = jnp.sum(jnp.where(first, 0.0, pairs), axis=1, keepdims=True)
        for r in range(8):
            total = total + jnp.where(label == even[r : r + 1, :], left[r : r + 1, :], 0.0)
            total = total + jnp.where(label == odd[r : r + 1, :], right[r : r + 1, :], 0.0)
        return total

    return lax.fori_loop(0, 16, column, jnp.zeros((8, 128), jnp.float32))


def gather_kernel(
    key_hbm, part_hbm, payload_hbm, probe_key_hbm, probe_part_hbm, g_ref, stat_ref,
    key_ref, part_ref, payload_ref, probe_key, probe_part, sums, parcels,
    loads, recv, pair_recv, send, stat_send, stat_recv,
):
    yh, z, yl, x, core = (lax.axis_index(a) for a in ALL)
    incoming = [
        pltpu.make_async_copy(src, dst, loads.at[n])
        for n, (src, dst) in enumerate(
            (
                (key_hbm, key_ref), (part_hbm, part_ref), (payload_hbm, payload_ref),
                (probe_key_hbm, probe_key), (probe_part_hbm, probe_part),
            )
        )
    ]
    for copy in incoming:
        copy.start()
    here = (x, yh * 2 + yl, z)

    def device(at, k):
        return (at[1] // 2, at[2], at[1] % 2, at[0], k)

    def slot(at, k):
        return (((at[1] % 2) * 4 + at[0]) * 2 + k) * 8 + (at[1] // 2) * 4 + at[2]

    def shifted(at, dim, delta):
        return tuple((v + delta) % 4 if d == dim else v for d, v in enumerate(at))

    def place(p, off):
        order = ORDERS[p]
        at = list(here)
        for level in range(3):
            at[order[level]] = (at[order[level]] + off[level]) % 4
        return slot(tuple(at), core)

    def block(p, index):
        return g_ref.at[index, pl.ds(CUTS[p][0], CUTS[p][1])]

    def push(p, off, level, delta):
        far = tuple((o - delta + 4) % 4 if n == level else o for n, o in enumerate(off))
        ref = block(p, place(p, off))
        pltpu.make_async_remote_copy(
            src_ref=ref, dst_ref=ref, send_sem=send.at[p], recv_sem=recv.at[p, far[0] * 16 + far[1] * 4 + far[2]],
            device_id=device(shifted(here, ORDERS[p][level], delta + 4), core), device_id_type=MESH,
        ).start()

    def pair(p, off):
        ref = block(p, place(p, off))
        pltpu.make_async_remote_copy(
            src_ref=ref, dst_ref=ref, send_sem=send.at[p], recv_sem=pair_recv.at[p],
            device_id=device(here, 1 - core), device_id_type=MESH,
        ).start()

    def arrive(p, off):
        ref = block(p, place(p, off))
        pltpu.make_async_remote_copy(
            src_ref=ref, dst_ref=ref, send_sem=send.at[p], recv_sem=recv.at[p, off[0] * 16 + off[1] * 4 + off[2]],
            device_id=device(here, 1 - core), device_id_type=MESH,
        ).wait_recv()

    barrier = pltpu.get_barrier_semaphore()
    for dim in range(3):
        for delta in (1, 3):
            pl.semaphore_signal(barrier, inc=1, device_id=device(shifted(here, dim, delta), core), device_id_type=MESH)
    pl.semaphore_signal(barrier, inc=1, device_id=device(here, 1 - core), device_id_type=MESH)

    for copy in incoming[:3]:
        copy.wait()
    table, side = table_of((yh * 4 + z) * 2, key_ref, part_ref, payload_ref)
    own = slot(here, core)
    g_ref[own, :128, :] = table
    g_ref[own, 128:, :] = side
    pl.semaphore_wait(barrier, 7)

    def both(p, off, level):
        push(p, off, level, 1)
        push(p, off, level, -1)

    for level in range(3):
        for p in range(3):
            both(p, (0, 0, 0), level)
    for p in range(3):
        pair(p, (0, 0, 0))
    for copy in incoming[3:]:
        copy.wait()
    live = live_rows(probe_key, probe_part)
    for p in range(3):
        arrive(p, (3, 0, 0))
        push(p, (3, 0, 0), 0, 1)
    for level in (1, 2):
        for p in range(3):
            both(p, (3, 0, 0), level)
    for p in range(3):
        arrive(p, (1, 0, 0))
        both(p, (1, 0, 0), 1)
        both(p, (1, 0, 0), 2)
    for p in range(3):
        arrive(p, (2, 0, 0))
        both(p, (2, 0, 0), 1)
        both(p, (2, 0, 0), 2)
    for p in range(3):
        for o in (3, 1, 2):
            pair(p, (o, 0, 0))

    def turn(i):
        return i + (i // 2) * (5 - 2 * i)

    def second(i, carry):
        da = turn(i)
        delta = 1 - 2 * (da % 2)
        for p in range(3):
            near = (4 - delta) % 4
            for o in (3, 1):
                arrive(p, (da, o, 0))
                both(p, (da, o, 0), 2)
            push(p, (da, near, 0), 1, delta)
            for o in (3, 1):
                pair(p, (da, o, 0))
        return carry

    def second_far(i, carry):
        da = turn(i)
        for p in range(3):
            arrive(p, (da, 2, 0))
            both(p, (da, 2, 0), 2)
            pair(p, (da, 2, 0))
        return carry

    def third(i, carry):
        da, db = turn(i % 4), turn(i // 4)
        delta = 1 - 2 * ((da + db) % 2)
        near = (4 - delta) % 4
        for p in range(3):
            for o in (3, 1):
                arrive(p, (da, db, o))
            push(p, (da, db, near), 2, delta)
            for o in (3, 1):
                pair(p, (da, db, o))
        return carry

    def third_far(i, carry):
        da, db = turn(i % 4), turn(i // 4)
        for p in range(3):
            arrive(p, (da, db, 2))
            pair(p, (da, db, 2))
        return carry

    lax.fori_loop(0, 4, second, 0)
    lax.fori_loop(0, 4, second_far, 0)
    lax.fori_loop(0, 16, third, 0)
    lax.fori_loop(0, 16, third_far, 0)
    for p in range(3):
        rows = pl.ds(CUTS[p][0], CUTS[p][1])
        landed = g_ref.at[pl.ds(0, 64), rows]
        pltpu.make_async_copy(landed, landed, pair_recv.at[p]).wait()

    now = jnp.concatenate([match_rows(probe_key, probe_part, g_ref), live], axis=0)
    first = 0
    for phase in range(4):
        sums[phase] = now
        sent = []
        for n in range(1 if phase == 0 else 3):
            target = device(here, 1 - core) if phase == 0 else device(shifted(here, phase - 1, n + 1), core)
            sent.append(
                pltpu.make_async_remote_copy(
                    src_ref=sums.at[phase], dst_ref=parcels.at[first + n], send_sem=stat_send.at[first + n],
                    recv_sem=stat_recv.at[first + n], device_id=target, device_id_type=MESH,
                )
            )
            sent[-1].start()
        for n, copy in enumerate(sent):
            copy.wait_recv()
            now = now + parcels[first + n]
        for copy in sent:
            copy.wait_send()
        first += len(sent)
    stat_ref[...] = now
    for p in range(3):
        rows = pl.ds(CUTS[p][0], CUTS[p][1])
        sent = g_ref.at[pl.ds(0, 127), rows]
        pltpu.make_async_copy(sent, sent, send.at[p]).wait()


def gather_tables(build_key, build_part, build_payload, probe_key, probe_part):
    hbm = pl.BlockSpec(memory_space=pltpu.HBM)
    vmem = pl.BlockSpec(memory_space=pltpu.VMEM)
    return pl.pallas_call(
        gather_kernel,
        out_shape=(
            jax.ShapeDtypeStruct((128, PIECE, 128), jnp.float32),
            jax.ShapeDtypeStruct((16, 128), jnp.float32),
        ),
        in_specs=[hbm] * 5,
        out_specs=(vmem, vmem),
        scratch_shapes=[
            pltpu.VMEM((1, 2, 128), jnp.int32),
            pltpu.SMEM((1, 2), jnp.int32),
            pltpu.VMEM((1, 2, 128, 128), jnp.float32),
            pltpu.VMEM((16, 8, 128), jnp.int32),
            pltpu.VMEM((16, 8, 128), jnp.int32),
            pltpu.VMEM((4, 16, 128), jnp.float32),
            pltpu.VMEM((10, 16, 128), jnp.float32),
            pltpu.SemaphoreType.DMA((5,)),
            pltpu.SemaphoreType.DMA((3, 64)),
            pltpu.SemaphoreType.DMA((3,)),
            pltpu.SemaphoreType.DMA((3,)),
            pltpu.SemaphoreType.DMA((10,)),
            pltpu.SemaphoreType.DMA((10,)),
        ],
        compiler_params=pltpu.CompilerParams(
            collective_id=0, has_side_effects=True, vmem_limit_bytes=16 * 1024 * 1024
        ),
        name="gather_tables",
    )(build_key, build_part, build_payload, probe_key, probe_part)


def join_kernel(key_ref, part_ref, g_ref, joined_ref, place_ref, table, hot):
    keys = key_ref[0].astype(jnp.float32)
    codes = coded(part_ref[0])
    tiles = []
    for r in range(8):
        piece = g_ref[r]
        high = piece.astype(jnp.bfloat16)
        low = (piece - high.astype(jnp.float32)).astype(jnp.bfloat16)
        lanes = pl.ds(r * 128, 128)
        table[0:128, lanes] = high[:128]
        table[128:256, lanes] = low[:128]
        table[256:272, lanes] = jnp.concatenate(
            [high[128:].astype(jnp.float32), low[128:].astype(jnp.float32)], axis=0
        ).astype(jnp.bfloat16)
        for t in range(2):
            tiles.append(jnp.broadcast_to(piece[132 + t : 133 + t, :], (16, 128)).astype(jnp.bfloat16))
    numbers = lax.broadcasted_iota(jnp.int32, (KEYS, 128), 0).astype(jnp.float32).astype(jnp.bfloat16)
    one, none = jnp.ones((KEYS, 128), jnp.bfloat16), jnp.zeros((KEYS, 128), jnp.bfloat16)
    for q2 in range(4):
        for h in range(2):
            q = q2 * 2 + h
            key_row = jnp.broadcast_to(keys[q : q + 1, :], (16, 128)).astype(jnp.bfloat16)
            key_hot = jnp.where(jnp.concatenate([key_row] * 4, axis=0) == numbers, one, none)
            code = jnp.broadcast_to(codes[q : q + 1, :], (16, 128)).astype(jnp.bfloat16)
            lanes = pl.ds(h * 128, 128)
            for t in range(16):
                same = jnp.where(code == tiles[t], one[:16], none[:16])
                hot[q2, t * KEYS : (t + 1) * KEYS, lanes] = key_hot * jnp.concatenate([same] * 4, axis=0)
        out = jnp.dot(table[...], hot[q2], preferred_element_type=jnp.float32)
        sums = out[:128] + out[128:256]
        joined_ref[0, q2 * 2] = sums[:, :128].T
        joined_ref[0, q2 * 2 + 1] = sums[:, 128:].T
        side = out[256:264] + out[264:272]
        for h in range(2):
            place_ref[0, q2 * 2 + h : q2 * 2 + h + 1, :] = side[0:1, h * 128 : (h + 1) * 128]


def join(probe_key, probe_part, tables):
    return pl.pallas_call(
        join_kernel,
        grid=(16,),
        out_shape=(
            jax.ShapeDtypeStruct((16, 8, 128, 128), jnp.float32),
            jax.ShapeDtypeStruct((16, 8, 128), jnp.float32),
        ),
        in_specs=[
            pl.BlockSpec((1, 8, 128), lambda c: (c, 0, 0)),
            pl.BlockSpec((1, 8, 128), lambda c: (c, 0, 0)),
            pl.BlockSpec((8, PIECE, 128), lambda c: (c, 0, 0)),
        ],
        out_specs=(
            pl.BlockSpec((1, 8, 128, 128), lambda c: (c, 0, 0, 0)),
            pl.BlockSpec((1, 8, 128), lambda c: (c, 0, 0)),
        ),
        scratch_shapes=[
            pltpu.VMEM((272, 1024), jnp.bfloat16),
            pltpu.VMEM((4, 1024, 256), jnp.bfloat16),
        ],
        compiler_params=pltpu.CompilerParams(vmem_limit_bytes=32 * 1024 * 1024),
        name="join",
    )(probe_key, probe_part, tables)


def local(build_key, build_part, build_payload, probe_key, probe_part):
    probe_key, probe_part = probe_key.reshape(16, 8, 128), probe_part.reshape(16, 8, 128)
    tables, stats = gather_tables(build_key, build_part, build_payload, probe_key, probe_part)
    joined, places = join(probe_key, probe_part, tables)
    rate = stats[:8].reshape(PARTS_SIZE) / jnp.maximum(stats[8:].reshape(PARTS_SIZE), 1.0)
    return (joined[None, None], places[None, None], rate)


def solution(mesh):
    finer = Mesh(mesh.devices.reshape(2, 4, 2, 4, 2), ALL)
    return jax.shard_map(
        local,
        mesh=finer,
        in_specs=(
            P(COL, ROW, None),
            P(COL, ROW),
            P(COL, ROW, None, None),
            P(ROW, COL, None, None, None),
            P(ROW, COL, None, None, None),
        ),
        out_specs=(P(ROW, COL, None, None, None, None), P(ROW, COL, None, None, None), P()),
        check_vma=False,
    )
```

```python
import functools

import jax
import jax.numpy as jnp
from jax import lax
from jax.experimental import pallas as pl
from jax.experimental.pallas import tpu as pltpu
from jax.sharding import Mesh
from jax.sharding import PartitionSpec as P

PARTS_SIZE = 1024
KEYS = 64
ROW = ("row_0", "row_1")
COL = ("col_0", "col_1", "col_2")
ALL = ROW + COL
MESH = pl.DeviceIdType.MESH

PIECE = 136
CUTS = ((0, 48), (48, 48), (96, 40))
ORDERS = ((0, 1, 2), (1, 2, 0), (2, 0, 1))


def coded(part):
    major = part // 128
    return (128 + part - major * 128).astype(jnp.float32) * (1 << major).astype(jnp.float32)


def table_of(tile_base, key_ref, part_ref, payload_ref):
    lane = lax.broadcasted_iota(jnp.int32, (8, 128), 1)
    sub = lax.broadcasted_iota(jnp.int32, (8, 128), 0)
    keys_col = lax.broadcasted_iota(jnp.int32, (KEYS, 128), 0)
    side_lhs = jnp.where(sub == 0, lane.astype(jnp.float32) / 2048.0, jnp.where(sub == 1, 1.0, 0.0))
    sums, sides = [], []
    for t in range(2):
        onehot = (keys_col == key_ref[0, t : t + 1, :]).astype(jnp.float32)
        sums.append(
            jnp.dot(onehot, payload_ref[0, t], precision=lax.Precision.HIGHEST, preferred_element_type=jnp.float32)
        )
        side = lax.dot_general(
            side_lhs, onehot, (((1,), (1,)), ((), ())), preferred_element_type=jnp.float32
        )
        start = (tile_base + t).astype(jnp.float32) / 16.0
        sides.append(side + jnp.where(sub[:, :KEYS] == 0, start * side[1:2, :], 0.0))
    table = jnp.concatenate(sums, axis=0).T
    side = jnp.concatenate(sides, axis=1)
    for t in range(2):
        part = part_ref[0, t]
        side = jnp.where(sub == 2 + t, part.astype(jnp.float32), side)
        side = jnp.where(sub == 4 + t, coded(jnp.full((8, 128), part)), side)
    return table, side


def live_rows(key_ref, part_ref):
    sub8 = lax.broadcasted_iota(jnp.int32, (8, 128), 0)
    sub128 = lax.broadcasted_iota(jnp.int32, (128, 128), 0)

    def column(c, total):
        keys, parts = key_ref[c], part_ref[c]
        major = parts // 128
        minor = parts - major * 128
        lhs, rhs = [], []
        for q in range(8):
            live = (sub8 == major[q : q + 1, :]) & (keys[q : q + 1, :] >= 0)
            lhs.append(jnp.where(live, 1.0, 0.0))
            rhs.append((sub128 == minor[q : q + 1, :]).astype(jnp.float32).astype(jnp.bfloat16))
        lhs = jnp.concatenate(lhs, axis=1).astype(jnp.bfloat16)
        rhs = jnp.concatenate(rhs, axis=1)
        return total + lax.dot_general(lhs, rhs, (((1,), (1,)), ((), ())), preferred_element_type=jnp.float32)

    def columns(i, total):
        for n in range(4):
            total = column(i * 4 + n, total)
        return total

    return lax.fori_loop(0, 4, columns, jnp.zeros((8, 128), jnp.float32))


def match_rows(key_ref, part_ref, g_ref):
    sub8 = lax.broadcasted_iota(jnp.int32, (8, 128), 0)
    lane8 = lax.broadcasted_iota(jnp.int32, (8, 128), 1)
    label = (sub8 * 128 + lane8).astype(jnp.float32)
    first = lane8 < KEYS
    sub128 = lax.broadcasted_iota(jnp.int32, (128, 128), 0)
    key_at = jnp.where(sub128 >= KEYS, sub128 - KEYS, sub128)

    def column(c, total):
        keys, parts = key_ref[c], part_ref[c].astype(jnp.float32)
        pieces = pl.ds(c * 8, 8)
        count, even, odd = g_ref[pieces, 129, :], g_ref[pieces, 130, :], g_ref[pieces, 131, :]
        lhs, rhs = [], []
        for q in range(8):
            row = parts[q : q + 1, :]
            lhs.append(jnp.concatenate([jnp.where(even == row, 1.0, 0.0), jnp.where(odd == row, 1.0, 0.0)], axis=0))
            rhs.append((key_at == keys[q : q + 1, :]).astype(jnp.float32).astype(jnp.bfloat16))
        lhs = jnp.concatenate(lhs, axis=1).astype(jnp.bfloat16)
        rhs = jnp.concatenate(rhs, axis=1)
        seen = lax.dot_general(lhs, rhs, (((1,), (1,)), ((), ())), preferred_element_type=jnp.float32)
        pairs = jnp.where(first, seen[:8], seen[8:]) * count
        left = jnp.sum(jnp.where(first, pairs, 0.0), axis=1, keepdims=True)
        right = jnp.sum(jnp.where(first, 0.0, pairs), axis=1, keepdims=True)
        for r in range(8):
            total = total + jnp.where(label == even[r : r + 1, :], left[r : r + 1, :], 0.0)
            total = total + jnp.where(label == odd[r : r + 1, :], right[r : r + 1, :], 0.0)
        return total

    def columns(i, total):
        for n in range(4):
            total = column(i * 4 + n, total)
        return total

    return lax.fori_loop(0, 4, columns, jnp.zeros((8, 128), jnp.float32))


def prepare(c, key_ref, part_ref, g_ref, table, hot):
    keys = key_ref[c].astype(jnp.float32)
    codes = coded(part_ref[c])
    tiles = []
    for r in range(8):
        piece = g_ref[c * 8 + r]
        high = piece.astype(jnp.bfloat16)
        low = (piece - high.astype(jnp.float32)).astype(jnp.bfloat16)
        lanes = pl.ds(r * 128, 128)
        table[0:128, lanes] = high[:128]
        table[128:256, lanes] = low[:128]
        table[256:272, lanes] = jnp.concatenate(
            [high[128:].astype(jnp.float32), low[128:].astype(jnp.float32)], axis=0
        ).astype(jnp.bfloat16)
        for t in range(2):
            tiles.append(jnp.broadcast_to(piece[132 + t : 133 + t, :], (16, 128)).astype(jnp.bfloat16))
    numbers = lax.broadcasted_iota(jnp.int32, (KEYS, 128), 0).astype(jnp.float32).astype(jnp.bfloat16)
    one, none = jnp.ones((KEYS, 128), jnp.bfloat16), jnp.zeros((KEYS, 128), jnp.bfloat16)
    for q in range(8):
        key_row = jnp.broadcast_to(keys[q : q + 1, :], (16, 128)).astype(jnp.bfloat16)
        key_hot = jnp.where(jnp.concatenate([key_row] * 4, axis=0) == numbers, one, none)
        code = jnp.broadcast_to(codes[q : q + 1, :], (16, 128)).astype(jnp.bfloat16)
        lanes = pl.ds(q % 2 * 128, 128)
        for t in range(16):
            same = jnp.where(code == tiles[t], one[:16], none[:16])
            hot[q // 2, t * KEYS : (t + 1) * KEYS, lanes] = key_hot * jnp.concatenate([same] * 4, axis=0)


def multiply(c, table, hot, joined_ref, place_ref):
    places = []
    for q2 in range(4):
        out = jnp.dot(table[...], hot[q2], preferred_element_type=jnp.float32)
        sums = out[:128] + out[128:256]
        joined_ref[c, q2 * 2] = sums[:, :128].T
        joined_ref[c, q2 * 2 + 1] = sums[:, 128:].T
        side = out[256:264] + out[264:272]
        for h in range(2):
            places.append(side[0:1, h * 128 : (h + 1) * 128])
    place_ref[c] = jnp.concatenate(places, axis=0)


def gather_kernel(
    key_hbm, part_hbm, payload_hbm, probe_key_hbm, probe_part_hbm, joined_ref, place_ref, stat_ref,
    g_ref, table_a, hot_a, table_b, hot_b, key_ref, part_ref, payload_ref, probe_key, probe_part, sums, parcels,
    loads, recv, pair_recv, send, stat_send, stat_recv,
):
    yh, z, yl, x, core = (lax.axis_index(a) for a in ALL)
    incoming = [
        pltpu.make_async_copy(src, dst, loads.at[n])
        for n, (src, dst) in enumerate(
            (
                (key_hbm, key_ref), (part_hbm, part_ref), (payload_hbm, payload_ref),
                (probe_key_hbm, probe_key), (probe_part_hbm, probe_part),
            )
        )
    ]
    for copy in incoming:
        copy.start()
    here = (x, yh * 2 + yl, z)

    def device(at, k):
        return (at[1] // 2, at[2], at[1] % 2, at[0], k)

    def slot(at, k):
        return (((at[1] % 2) * 4 + at[0]) * 2 + k) * 8 + (at[1] // 2) * 4 + at[2]

    def shifted(at, dim, delta):
        return tuple((v + delta) % 4 if d == dim else v for d, v in enumerate(at))

    def place(p, off):
        order = ORDERS[p]
        at = list(here)
        for level in range(3):
            at[order[level]] = (at[order[level]] + off[level]) % 4
        return slot(tuple(at), core)

    def block(p, index):
        return g_ref.at[index, pl.ds(CUTS[p][0], CUTS[p][1])]

    def push(p, off, level, delta):
        far = tuple((o - delta + 4) % 4 if n == level else o for n, o in enumerate(off))
        ref = block(p, place(p, off))
        pltpu.make_async_remote_copy(
            src_ref=ref, dst_ref=ref, send_sem=send.at[p], recv_sem=recv.at[p, far[0] * 16 + far[1] * 4 + far[2]],
            device_id=device(shifted(here, ORDERS[p][level], delta + 4), core), device_id_type=MESH,
        ).start()

    def pair(p, off):
        ref = block(p, place(p, off))
        pltpu.make_async_remote_copy(
            src_ref=ref, dst_ref=ref, send_sem=send.at[p], recv_sem=pair_recv.at[p],
            device_id=device(here, 1 - core), device_id_type=MESH,
        ).start()

    def arrive(p, off):
        ref = block(p, place(p, off))
        pltpu.make_async_remote_copy(
            src_ref=ref, dst_ref=ref, send_sem=send.at[p], recv_sem=recv.at[p, off[0] * 16 + off[1] * 4 + off[2]],
            device_id=device(here, 1 - core), device_id_type=MESH,
        ).wait_recv()

    barrier = pltpu.get_barrier_semaphore()
    for dim in range(3):
        for delta in (1, 3):
            pl.semaphore_signal(barrier, inc=1, device_id=device(shifted(here, dim, delta), core), device_id_type=MESH)
    pl.semaphore_signal(barrier, inc=1, device_id=device(here, 1 - core), device_id_type=MESH)

    for copy in incoming[:3]:
        copy.wait()
    table, side = table_of((yh * 4 + z) * 2, key_ref, part_ref, payload_ref)
    own = slot(here, core)
    g_ref[own, :128, :] = table
    g_ref[own, 128:, :] = side
    pl.semaphore_wait(barrier, 7)

    def both(p, off, level):
        push(p, off, level, 1)
        push(p, off, level, -1)

    for level in range(3):
        for p in range(3):
            both(p, (0, 0, 0), level)
    for p in range(3):
        pair(p, (0, 0, 0))
    for copy in incoming[3:]:
        copy.wait()
    live = live_rows(probe_key, probe_part)
    for p in range(3):
        arrive(p, (3, 0, 0))
        push(p, (3, 0, 0), 0, 1)
    for level in (1, 2):
        for p in range(3):
            both(p, (3, 0, 0), level)
    for p in range(3):
        arrive(p, (1, 0, 0))
        both(p, (1, 0, 0), 1)
        both(p, (1, 0, 0), 2)
    for p in range(3):
        arrive(p, (2, 0, 0))
        both(p, (2, 0, 0), 1)
        both(p, (2, 0, 0), 2)
    for p in range(3):
        for o in (3, 1, 2):
            pair(p, (o, 0, 0))

    def turn(i):
        return i + (i // 2) * (5 - 2 * i)

    def second(i, carry):
        da = turn(i)
        delta = 1 - 2 * (da % 2)
        for p in range(3):
            near = (4 - delta) % 4
            for o in (3, 1):
                arrive(p, (da, o, 0))
                both(p, (da, o, 0), 2)
            push(p, (da, near, 0), 1, delta)
            for o in (3, 1):
                pair(p, (da, o, 0))
        return carry

    def second_far(i, carry):
        da = turn(i)
        for p in range(3):
            arrive(p, (da, 2, 0))
            both(p, (da, 2, 0), 2)
            pair(p, (da, 2, 0))
        return carry

    def third(i, carry):
        da, db = turn(i % 4), turn(i // 4)
        delta = 1 - 2 * ((da + db) % 2)
        near = (4 - delta) % 4
        for p in range(3):
            for o in (3, 1):
                arrive(p, (da, db, o))
            push(p, (da, db, near), 2, delta)
            for o in (3, 1):
                pair(p, (da, db, o))
        return carry

    def third_far(i, carry):
        da, db = turn(i % 4), turn(i // 4)
        for p in range(3):
            arrive(p, (da, db, 2))
            pair(p, (da, db, 2))
        return carry

    lax.fori_loop(0, 4, second, 0)
    lax.fori_loop(0, 4, second_far, 0)
    lax.fori_loop(0, 16, third, 0)
    lax.fori_loop(0, 16, third_far, 0)
    for p in range(3):
        rows = pl.ds(CUTS[p][0], CUTS[p][1])
        landed = g_ref.at[pl.ds(0, 64), rows]
        pltpu.make_async_copy(landed, landed, pair_recv.at[p]).wait()

    def parcels_of(phase):
        copies = []
        for n in range(1 if phase == 0 else 3):
            target = device(here, 1 - core) if phase == 0 else device(shifted(here, phase - 1, n + 1), core)
            at = 3 * phase - 2 + n if phase else 0
            copies.append(
                pltpu.make_async_remote_copy(
                    src_ref=sums.at[phase], dst_ref=parcels.at[at], send_sem=stat_send.at[at],
                    recv_sem=stat_recv.at[at], device_id=target, device_id_type=MESH,
                )
            )
        return copies

    def begin(phase):
        for copy in parcels_of(phase):
            copy.start()

    def finish(phase):
        now = sums[phase]
        for n, copy in enumerate(parcels_of(phase)):
            copy.wait_recv()
            now = now + parcels[3 * phase - 2 + n if phase else 0]
        for copy in parcels_of(phase):
            copy.wait_send()
        return now

    sums[0] = jnp.concatenate([match_rows(probe_key, probe_part, g_ref), live], axis=0)
    begin(0)
    prepare(0, probe_key, probe_part, g_ref, table_a, hot_a)

    def joins(i, carry):
        for phase in range(1, 4):
            @pl.when(i == 2 * phase)
            def _():
                sums[phase] = finish(phase - 1)
                begin(phase)

        prepare(2 * i + 1, probe_key, probe_part, g_ref, table_b, hot_b)
        multiply(2 * i, table_a, hot_a, joined_ref, place_ref)
        prepare(jnp.minimum(2 * i + 2, 15), probe_key, probe_part, g_ref, table_a, hot_a)
        multiply(2 * i + 1, table_b, hot_b, joined_ref, place_ref)
        return carry

    lax.fori_loop(0, 8, joins, 0)
    stat_ref[...] = finish(3)
    for p in range(3):
        rows = pl.ds(CUTS[p][0], CUTS[p][1])
        sent = g_ref.at[pl.ds(0, 127), rows]
        pltpu.make_async_copy(sent, sent, send.at[p]).wait()


def gather_and_join(build_key, build_part, build_payload, probe_key, probe_part):
    hbm = pl.BlockSpec(memory_space=pltpu.HBM)
    vmem = pl.BlockSpec(memory_space=pltpu.VMEM)
    return pl.pallas_call(
        gather_kernel,
        out_shape=(
            jax.ShapeDtypeStruct((16, 8, 128, 128), jnp.float32),
            jax.ShapeDtypeStruct((16, 8, 128), jnp.float32),
            jax.ShapeDtypeStruct((16, 128), jnp.float32),
        ),
        in_specs=[hbm] * 5,
        out_specs=(vmem, vmem, vmem),
        scratch_shapes=[
            pltpu.VMEM((128, PIECE, 128), jnp.float32),
            pltpu.VMEM((272, 1024), jnp.bfloat16),
            pltpu.VMEM((4, 1024, 256), jnp.bfloat16),
            pltpu.VMEM((272, 1024), jnp.bfloat16),
            pltpu.VMEM((4, 1024, 256), jnp.bfloat16),
            pltpu.VMEM((1, 2, 128), jnp.int32),
            pltpu.SMEM((1, 2), jnp.int32),
            pltpu.VMEM((1, 2, 128, 128), jnp.float32),
            pltpu.VMEM((16, 8, 128), jnp.int32),
            pltpu.VMEM((16, 8, 128), jnp.int32),
            pltpu.VMEM((4, 16, 128), jnp.float32),
            pltpu.VMEM((10, 16, 128), jnp.float32),
            pltpu.SemaphoreType.DMA((5,)),
            pltpu.SemaphoreType.DMA((3, 64)),
            pltpu.SemaphoreType.DMA((3,)),
            pltpu.SemaphoreType.DMA((3,)),
            pltpu.SemaphoreType.DMA((10,)),
            pltpu.SemaphoreType.DMA((10,)),
        ],
        compiler_params=pltpu.CompilerParams(
            collective_id=0, has_side_effects=True, vmem_limit_bytes=40 * 1024 * 1024
        ),
        name="gather_and_join",
    )(
        *(
            pltpu.with_memory_space_constraint(a, pltpu.HBM)
            for a in (build_key, build_part, build_payload, probe_key, probe_part)
        )
    )


def local(build_key, build_part, build_payload, probe_key, probe_part):
    probe_key, probe_part = probe_key.reshape(16, 8, 128), probe_part.reshape(16, 8, 128)
    joined, places, stats = gather_and_join(build_key, build_part, build_payload, probe_key, probe_part)
    rate = stats[:8].reshape(PARTS_SIZE) / jnp.maximum(stats[8:].reshape(PARTS_SIZE), 1.0)
    return (joined[None, None], places[None, None], rate)


def solution(mesh):
    finer = Mesh(mesh.devices.reshape(2, 4, 2, 4, 2), ALL)
    return jax.shard_map(
        local,
        mesh=finer,
        in_specs=(
            P(COL, ROW, None),
            P(COL, ROW),
            P(COL, ROW, None, None),
            P(ROW, COL, None, None, None),
            P(ROW, COL, None, None, None),
        ),
        out_specs=(P(ROW, COL, None, None, None, None), P(ROW, COL, None, None, None), P()),
        check_vma=False,
    )
```

```python
import functools

import jax
import jax.numpy as jnp
from jax import lax
from jax.experimental import pallas as pl
from jax.experimental.pallas import tpu as pltpu
from jax.sharding import Mesh
from jax.sharding import PartitionSpec as P

PARTS_SIZE = 1024
KEYS = 64
EARLY = 14
ROW = ("row_0", "row_1")
COL = ("col_0", "col_1", "col_2")
ALL = ROW + COL
MESH = pl.DeviceIdType.MESH

PIECE = 136
CUTS = ((0, 48), (48, 48), (96, 40))
ORDERS = ((0, 1, 2), (1, 2, 0), (2, 0, 1))


def coded(part):
    major = part // 128
    return (128 + part - major * 128).astype(jnp.float32) * (1 << major).astype(jnp.float32)


def table_of(tile_base, key_ref, part_ref, payload_ref):
    lane = lax.broadcasted_iota(jnp.int32, (8, 128), 1)
    sub = lax.broadcasted_iota(jnp.int32, (8, 128), 0)
    keys_col = lax.broadcasted_iota(jnp.int32, (KEYS, 128), 0)
    side_lhs = jnp.where(sub == 0, lane.astype(jnp.float32) / 2048.0, jnp.where(sub == 1, 1.0, 0.0))
    sums, sides = [], []
    for t in range(2):
        onehot = (keys_col == key_ref[0, t : t + 1, :]).astype(jnp.float32)
        sums.append(
            jnp.dot(onehot, payload_ref[0, t], precision=lax.Precision.HIGHEST, preferred_element_type=jnp.float32)
        )
        side = lax.dot_general(
            side_lhs, onehot, (((1,), (1,)), ((), ())), preferred_element_type=jnp.float32
        )
        start = (tile_base + t).astype(jnp.float32) / 16.0
        sides.append(side + jnp.where(sub[:, :KEYS] == 0, start * side[1:2, :], 0.0))
    table = jnp.concatenate(sums, axis=0).T
    side = jnp.concatenate(sides, axis=1)
    for t in range(2):
        part = part_ref[0, t]
        side = jnp.where(sub == 2 + t, part.astype(jnp.float32), side)
        side = jnp.where(sub == 4 + t, coded(jnp.full((8, 128), part)), side)
    return table, side


def live_rows(key_ref, part_ref):
    sub8 = lax.broadcasted_iota(jnp.int32, (8, 128), 0)
    sub128 = lax.broadcasted_iota(jnp.int32, (128, 128), 0)

    def column(c, total):
        keys, parts = key_ref[c], part_ref[c]
        major = parts // 128
        minor = parts - major * 128
        lhs, rhs = [], []
        for q in range(8):
            live = (sub8 == major[q : q + 1, :]) & (keys[q : q + 1, :] >= 0)
            lhs.append(jnp.where(live, 1.0, 0.0))
            rhs.append((sub128 == minor[q : q + 1, :]).astype(jnp.float32).astype(jnp.bfloat16))
        lhs = jnp.concatenate(lhs, axis=1).astype(jnp.bfloat16)
        rhs = jnp.concatenate(rhs, axis=1)
        return total + lax.dot_general(lhs, rhs, (((1,), (1,)), ((), ())), preferred_element_type=jnp.float32)

    def columns(i, total):
        for n in range(4):
            total = column(i * 4 + n, total)
        return total

    return lax.fori_loop(0, 4, columns, jnp.zeros((8, 128), jnp.float32))


def match_rows(key_ref, part_ref, g_ref):
    sub8 = lax.broadcasted_iota(jnp.int32, (8, 128), 0)
    lane8 = lax.broadcasted_iota(jnp.int32, (8, 128), 1)
    label = (sub8 * 128 + lane8).astype(jnp.float32)
    first = lane8 < KEYS
    sub128 = lax.broadcasted_iota(jnp.int32, (128, 128), 0)
    key_at = jnp.where(sub128 >= KEYS, sub128 - KEYS, sub128)

    def column(c, total):
        keys, parts = key_ref[c], part_ref[c].astype(jnp.float32)
        pieces = pl.ds(c * 8, 8)
        count, even, odd = g_ref[pieces, 129, :], g_ref[pieces, 130, :], g_ref[pieces, 131, :]
        lhs, rhs = [], []
        for q in range(8):
            row = parts[q : q + 1, :]
            lhs.append(jnp.concatenate([jnp.where(even == row, 1.0, 0.0), jnp.where(odd == row, 1.0, 0.0)], axis=0))
            rhs.append((key_at == keys[q : q + 1, :]).astype(jnp.float32).astype(jnp.bfloat16))
        lhs = jnp.concatenate(lhs, axis=1).astype(jnp.bfloat16)
        rhs = jnp.concatenate(rhs, axis=1)
        seen = lax.dot_general(lhs, rhs, (((1,), (1,)), ((), ())), preferred_element_type=jnp.float32)
        pairs = jnp.where(first, seen[:8], seen[8:]) * count
        left = jnp.sum(jnp.where(first, pairs, 0.0), axis=1, keepdims=True)
        right = jnp.sum(jnp.where(first, 0.0, pairs), axis=1, keepdims=True)
        for r in range(8):
            total = total + jnp.where(label == even[r : r + 1, :], left[r : r + 1, :], 0.0)
            total = total + jnp.where(label == odd[r : r + 1, :], right[r : r + 1, :], 0.0)
        return total

    def columns(i, total):
        for n in range(4):
            total = column(i * 4 + n, total)
        return total

    return lax.fori_loop(0, 4, columns, jnp.zeros((8, 128), jnp.float32))


def prepare(c, key_ref, part_ref, g_ref, table, hot, column=None):
    column = c if column is None else column
    keys = key_ref[c].astype(jnp.float32)
    codes = coded(part_ref[c])
    tiles = []
    for r in range(8):
        piece = g_ref[column * 8 + r]
        high = piece.astype(jnp.bfloat16)
        low = (piece - high.astype(jnp.float32)).astype(jnp.bfloat16)
        lanes = pl.ds(r * 128, 128)
        table[0:128, lanes] = high[:128]
        table[128:256, lanes] = low[:128]
        table[256:272, lanes] = jnp.concatenate(
            [high[128:].astype(jnp.float32), low[128:].astype(jnp.float32)], axis=0
        ).astype(jnp.bfloat16)
        for t in range(2):
            tiles.append(jnp.broadcast_to(piece[132 + t : 133 + t, :], (16, 128)).astype(jnp.bfloat16))
    numbers = lax.broadcasted_iota(jnp.int32, (KEYS, 128), 0).astype(jnp.float32).astype(jnp.bfloat16)
    one, none = jnp.ones((KEYS, 128), jnp.bfloat16), jnp.zeros((KEYS, 128), jnp.bfloat16)
    for q in range(8):
        key_row = jnp.broadcast_to(keys[q : q + 1, :], (16, 128)).astype(jnp.bfloat16)
        key_hot = jnp.where(jnp.concatenate([key_row] * 4, axis=0) == numbers, one, none)
        code = jnp.broadcast_to(codes[q : q + 1, :], (16, 128)).astype(jnp.bfloat16)
        lanes = pl.ds(q % 2 * 128, 128)
        for t in range(16):
            same = jnp.where(code == tiles[t], one[:16], none[:16])
            hot[q // 2, t * KEYS : (t + 1) * KEYS, lanes] = key_hot * jnp.concatenate([same] * 4, axis=0)


def multiply(c, table, hot, joined_ref, place_ref):
    places = []
    for q2 in range(4):
        out = jnp.dot(table[...], hot[q2], preferred_element_type=jnp.float32)
        sums = out[:128] + out[128:256]
        joined_ref[c, q2 * 2] = sums[:, :128].T
        joined_ref[c, q2 * 2 + 1] = sums[:, 128:].T
        side = out[256:264] + out[264:272]
        for h in range(2):
            places.append(side[0:1, h * 128 : (h + 1) * 128])
    place_ref[c] = jnp.concatenate(places, axis=0)


def gather_kernel(
    key_hbm, part_hbm, payload_hbm, probe_key_hbm, probe_part_hbm, joined_ref, place_ref, stat_ref, g_ref,
    table_a, hot_a, table_b, hot_b, key_ref, part_ref, payload_ref, probe_key, probe_part, sums, parcels,
    loads, recv, pair_recv, send, stat_send, stat_recv,
):
    yh, z, yl, x, core = (lax.axis_index(a) for a in ALL)
    incoming = [
        pltpu.make_async_copy(src, dst, loads.at[n])
        for n, (src, dst) in enumerate(
            (
                (key_hbm, key_ref), (part_hbm, part_ref), (payload_hbm, payload_ref),
                (probe_key_hbm, probe_key), (probe_part_hbm, probe_part),
            )
        )
    ]
    for copy in incoming:
        copy.start()
    here = (x, yh * 2 + yl, z)

    def device(at, k):
        return (at[1] // 2, at[2], at[1] % 2, at[0], k)

    def slot(at, k):
        return (((at[1] % 2) * 4 + at[0]) * 2 + k) * 8 + (at[1] // 2) * 4 + at[2]

    def shifted(at, dim, delta):
        return tuple((v + delta) % 4 if d == dim else v for d, v in enumerate(at))

    def place(p, off):
        order = ORDERS[p]
        at = list(here)
        for level in range(3):
            at[order[level]] = (at[order[level]] + off[level]) % 4
        return slot(tuple(at), core)

    def block(p, index):
        return g_ref.at[index, pl.ds(CUTS[p][0], CUTS[p][1])]

    def push(p, off, level, delta):
        far = tuple((o - delta + 4) % 4 if n == level else o for n, o in enumerate(off))
        ref = block(p, place(p, off))
        pltpu.make_async_remote_copy(
            src_ref=ref, dst_ref=ref, send_sem=send.at[p], recv_sem=recv.at[p, far[0] * 16 + far[1] * 4 + far[2]],
            device_id=device(shifted(here, ORDERS[p][level], delta + 4), core), device_id_type=MESH,
        ).start()

    def pair(p, off):
        ref = block(p, place(p, off))
        pltpu.make_async_remote_copy(
            src_ref=ref, dst_ref=ref, send_sem=send.at[p], recv_sem=pair_recv.at[p],
            device_id=device(here, 1 - core), device_id_type=MESH,
        ).start()

    def arrive(p, off):
        ref = block(p, place(p, off))
        pltpu.make_async_remote_copy(
            src_ref=ref, dst_ref=ref, send_sem=send.at[p], recv_sem=recv.at[p, off[0] * 16 + off[1] * 4 + off[2]],
            device_id=device(here, 1 - core), device_id_type=MESH,
        ).wait_recv()

    barrier = pltpu.get_barrier_semaphore()
    for dim in range(3):
        for delta in (1, 2, 3):
            pl.semaphore_signal(barrier, inc=1, device_id=device(shifted(here, dim, delta), core), device_id_type=MESH)
    pl.semaphore_signal(barrier, inc=1, device_id=device(here, 1 - core), device_id_type=MESH)

    for copy in incoming[:3]:
        copy.wait()
    table, side = table_of((yh * 4 + z) * 2, key_ref, part_ref, payload_ref)
    own = slot(here, core)
    g_ref[own, :128, :] = table
    g_ref[own, 128:, :] = side
    pl.semaphore_wait(barrier, 10)

    def spread(p, off, level):
        for delta in (2, 1, -1) if level < 2 else (1, -1):
            push(p, off, level, delta)

    for level in range(3):
        for p in range(3):
            spread(p, (0, 0, 0), level)
    for p in range(3):
        pair(p, (0, 0, 0))
    for copy in incoming[3:]:
        copy.wait()
    live = live_rows(probe_key, probe_part)
    for o in (3, 1, 2):
        for p in range(3):
            arrive(p, (o, 0, 0))
            spread(p, (o, 0, 0), 1)
            spread(p, (o, 0, 0), 2)
    for p in range(3):
        for o in (3, 1, 2):
            pair(p, (o, 0, 0))

    def turn(i):
        return i + (i // 2) * (5 - 2 * i)

    def second(i, carry):
        da = turn(i)
        for p in range(3):
            for o in (3, 1):
                arrive(p, (da, o, 0))
                spread(p, (da, o, 0), 2)
                pair(p, (da, o, 0))
        return carry

    def second_far(i, carry):
        da = turn(i)
        for p in range(3):
            arrive(p, (da, 2, 0))
            spread(p, (da, 2, 0), 2)
            pair(p, (da, 2, 0))
        return carry

    def third(i, carry):
        da, db = turn(i % 4), turn(i // 4)
        delta = 1 - 2 * ((da + db) % 2)
        near = (4 - delta) % 4
        for p in range(3):
            for o in (3, 1):
                arrive(p, (da, db, o))
            push(p, (da, db, near), 2, delta)
            for o in (3, 1):
                pair(p, (da, db, o))
        return carry

    def third_far(i, carry):
        da, db = turn(i % 4), turn(i // 4)
        for p in range(3):
            arrive(p, (da, db, 2))
            pair(p, (da, db, 2))
        return carry

    lax.fori_loop(0, 4, second, 0)
    lax.fori_loop(0, 4, second_far, 0)
    lax.fori_loop(0, 16, third, 0)
    lax.fori_loop(0, 16, third_far, 0)
    for p in range(3):
        rows = pl.ds(CUTS[p][0], CUTS[p][1])
        landed = g_ref.at[pl.ds(0, 64), rows]
        pltpu.make_async_copy(landed, landed, pair_recv.at[p]).wait()

    def parcels_of(phase):
        copies = []
        for n in range(1 if phase == 0 else 3):
            target = device(here, 1 - core) if phase == 0 else device(shifted(here, phase - 1, n + 1), core)
            at = 3 * phase - 2 + n if phase else 0
            copies.append(
                pltpu.make_async_remote_copy(
                    src_ref=sums.at[phase], dst_ref=parcels.at[at], send_sem=stat_send.at[at],
                    recv_sem=stat_recv.at[at], device_id=target, device_id_type=MESH,
                )
            )
        return copies

    def begin(phase):
        for copy in parcels_of(phase):
            copy.start()

    def finish(phase):
        now = sums[phase]
        for n, copy in enumerate(parcels_of(phase)):
            copy.wait_recv()
            now = now + parcels[3 * phase - 2 + n if phase else 0]
        for copy in parcels_of(phase):
            copy.wait_send()
        return now

    sums[0] = jnp.concatenate([match_rows(probe_key, probe_part, g_ref), live], axis=0)
    begin(0)
    prepare(0, probe_key, probe_part, g_ref, table_a, hot_a)

    def joins(i, carry):
        for phase in range(1, 4):
            @pl.when(i == 2 * phase - (phase == 1))
            def _():
                sums[phase] = finish(phase - 1)
                begin(phase)

        prepare(2 * i + 1, probe_key, probe_part, g_ref, table_b, hot_b)
        multiply(2 * i, table_a, hot_a, joined_ref, place_ref)
        prepare(jnp.minimum(2 * i + 2, EARLY - 1), probe_key, probe_part, g_ref, table_a, hot_a)
        multiply(2 * i + 1, table_b, hot_b, joined_ref, place_ref)
        return carry

    lax.fori_loop(0, EARLY // 2, joins, 0)
    stat_ref[...] = finish(3)
    for p in range(3):
        rows = pl.ds(CUTS[p][0], CUTS[p][1])
        sent = g_ref.at[pl.ds(0, 127), rows]
        pltpu.make_async_copy(sent, sent, send.at[p]).wait()


def gather_and_join(build_key, build_part, build_payload, probe_key, probe_part):
    hbm = pl.BlockSpec(memory_space=pltpu.HBM)
    vmem = pl.BlockSpec(memory_space=pltpu.VMEM)
    return pl.pallas_call(
        gather_kernel,
        out_shape=(
            jax.ShapeDtypeStruct((EARLY, 8, 128, 128), jnp.float32),
            jax.ShapeDtypeStruct((EARLY, 8, 128), jnp.float32),
            jax.ShapeDtypeStruct((16, 128), jnp.float32),
            jax.ShapeDtypeStruct((128, PIECE, 128), jnp.float32),
        ),
        in_specs=[hbm] * 5,
        out_specs=(vmem, vmem, vmem, vmem),
        scratch_shapes=[
            pltpu.VMEM((272, 1024), jnp.bfloat16),
            pltpu.VMEM((4, 1024, 256), jnp.bfloat16),
            pltpu.VMEM((272, 1024), jnp.bfloat16),
            pltpu.VMEM((4, 1024, 256), jnp.bfloat16),
            pltpu.VMEM((1, 2, 128), jnp.int32),
            pltpu.SMEM((1, 2), jnp.int32),
            pltpu.VMEM((1, 2, 128, 128), jnp.float32),
            pltpu.VMEM((16, 8, 128), jnp.int32),
            pltpu.VMEM((16, 8, 128), jnp.int32),
            pltpu.VMEM((4, 16, 128), jnp.float32),
            pltpu.VMEM((10, 16, 128), jnp.float32),
            pltpu.SemaphoreType.DMA((5,)),
            pltpu.SemaphoreType.DMA((3, 64)),
            pltpu.SemaphoreType.DMA((3,)),
            pltpu.SemaphoreType.DMA((3,)),
            pltpu.SemaphoreType.DMA((10,)),
            pltpu.SemaphoreType.DMA((10,)),
        ],
        compiler_params=pltpu.CompilerParams(
            collective_id=0, has_side_effects=True, vmem_limit_bytes=20 * 1024 * 1024
        ),
        name="gather_and_join",
    )(
        *(
            pltpu.with_memory_space_constraint(a, pltpu.HBM)
            for a in (build_key, build_part, build_payload, probe_key, probe_part)
        )
    )


def finish_kernel(
    key_hbm, part_hbm, early_ref, early_place_ref, stat_ref, g_ref, joined_hbm, place_hbm, rate_hbm,
    probe_key, probe_part, joined_ref, place_ref, rate_ref, table_a, hot_a, table_b, hot_b, loads, stores,
):
    late = 16 - EARLY
    incoming = [
        pltpu.make_async_copy(src.at[pl.ds(EARLY, late)], dst, loads.at[n])
        for n, (src, dst) in enumerate(((key_hbm, probe_key), (part_hbm, probe_part)))
    ]
    for copy in incoming:
        copy.start()
    outgoing = [
        pltpu.make_async_copy(early_ref, joined_hbm.at[pl.ds(0, EARLY)], stores.at[0]),
        pltpu.make_async_copy(early_place_ref, place_hbm.at[pl.ds(0, EARLY)], stores.at[1]),
    ]
    for copy in outgoing:
        copy.start()
    rate_ref[...] = stat_ref[0:8, :] / jnp.maximum(stat_ref[8:16, :], 1.0)
    outgoing.append(pltpu.make_async_copy(rate_ref, rate_hbm, stores.at[2]))
    outgoing[-1].start()
    for copy in incoming:
        copy.wait()
    buffers = ((table_a, hot_a), (table_b, hot_b))

    def ready(n):
        prepare(n, probe_key, probe_part, g_ref, *buffers[n % 2], EARLY + n)

    ready(0)
    for n in range(late):
        if n + 1 < late:
            ready(n + 1)
        multiply(n, *buffers[n % 2], joined_ref, place_ref)
        outgoing.append(pltpu.make_async_copy(joined_ref.at[n], joined_hbm.at[EARLY + n], stores.at[3 + n]))
        outgoing[-1].start()
    outgoing.append(pltpu.make_async_copy(place_ref, place_hbm.at[pl.ds(EARLY, late)], stores.at[3 + late]))
    outgoing[-1].start()
    for copy in outgoing:
        copy.wait()


def finish_join(probe_key, probe_part, early, early_places, stats, tables):
    hbm = pl.BlockSpec(memory_space=pltpu.HBM)
    vmem = pl.BlockSpec(memory_space=pltpu.VMEM)
    late = 16 - EARLY
    return pl.pallas_call(
        finish_kernel,
        out_shape=(
            jax.ShapeDtypeStruct((16, 8, 128, 128), jnp.float32),
            jax.ShapeDtypeStruct((16, 8, 128), jnp.float32),
            jax.ShapeDtypeStruct((8, 128), jnp.float32),
        ),
        in_specs=[hbm, hbm, vmem, vmem, vmem, vmem],
        out_specs=(hbm, hbm, hbm),
        scratch_shapes=[
            pltpu.VMEM((late, 8, 128), jnp.int32),
            pltpu.VMEM((late, 8, 128), jnp.int32),
            pltpu.VMEM((late, 8, 128, 128), jnp.float32),
            pltpu.VMEM((late, 8, 128), jnp.float32),
            pltpu.VMEM((8, 128), jnp.float32),
            pltpu.VMEM((272, 1024), jnp.bfloat16),
            pltpu.VMEM((4, 1024, 256), jnp.bfloat16),
            pltpu.VMEM((272, 1024), jnp.bfloat16),
            pltpu.VMEM((4, 1024, 256), jnp.bfloat16),
            pltpu.SemaphoreType.DMA((2,)),
            pltpu.SemaphoreType.DMA((4 + late,)),
        ],
        compiler_params=pltpu.CompilerParams(vmem_limit_bytes=24 * 1024 * 1024),
        name="finish_join",
    )(
        *(pltpu.with_memory_space_constraint(a, pltpu.HBM) for a in (probe_key, probe_part)),
        early, early_places, stats, tables,
    )


def local(build_key, build_part, build_payload, probe_key, probe_part):
    probe_key, probe_part = probe_key.reshape(16, 8, 128), probe_part.reshape(16, 8, 128)
    early, early_places, stats, tables = gather_and_join(build_key, build_part, build_payload, probe_key, probe_part)
    joined, places, rate = finish_join(probe_key, probe_part, early, early_places, stats, tables)
    return (joined[None, None], places[None, None], rate.reshape(PARTS_SIZE))


def solution(mesh):
    finer = Mesh(mesh.devices.reshape(2, 4, 2, 4, 2), ALL)
    return jax.shard_map(
        local,
        mesh=finer,
        in_specs=(
            P(COL, ROW, None),
            P(COL, ROW),
            P(COL, ROW, None, None),
            P(ROW, COL, None, None, None),
            P(ROW, COL, None, None, None),
        ),
        out_specs=(P(ROW, COL, None, None, None, None), P(ROW, COL, None, None, None), P()),
        check_vma=False,
    )
```

```python
import functools

import jax
import jax.numpy as jnp
from jax import lax
from jax.experimental import pallas as pl
from jax.experimental.pallas import tpu as pltpu
from jax.sharding import Mesh
from jax.sharding import PartitionSpec as P

PARTS_SIZE = 1024
KEYS = 64
EARLY = 14
ROW = ("row_0", "row_1")
COL = ("col_0", "col_1", "col_2")
ALL = ROW + COL
MESH = pl.DeviceIdType.MESH

PIECE = 136
CUTS = ((0, 48), (48, 48), (96, 40))
ORDERS = ((0, 1, 2), (1, 2, 0), (2, 0, 1))


def coded(part):
    major = part // 128
    return (128 + part - major * 128).astype(jnp.float32) * (1 << major).astype(jnp.float32)


def table_of(tile_base, key_ref, part_ref, payload_ref):
    lane = lax.broadcasted_iota(jnp.int32, (8, 128), 1)
    sub = lax.broadcasted_iota(jnp.int32, (8, 128), 0)
    keys_col = lax.broadcasted_iota(jnp.int32, (KEYS, 128), 0)
    side_lhs = jnp.where(sub == 0, lane.astype(jnp.float32) / 2048.0, jnp.where(sub == 1, 1.0, 0.0))
    sums, sides = [], []
    for t in range(2):
        onehot = (keys_col == key_ref[0, t : t + 1, :]).astype(jnp.float32)
        sums.append(
            jnp.dot(onehot, payload_ref[0, t], precision=lax.Precision.HIGHEST, preferred_element_type=jnp.float32)
        )
        side = lax.dot_general(
            side_lhs, onehot, (((1,), (1,)), ((), ())), preferred_element_type=jnp.float32
        )
        start = (tile_base + t).astype(jnp.float32) / 16.0
        sides.append(side + jnp.where(sub[:, :KEYS] == 0, start * side[1:2, :], 0.0))
    table = jnp.concatenate(sums, axis=0).T
    side = jnp.concatenate(sides, axis=1)
    for t in range(2):
        part = part_ref[0, t]
        side = jnp.where(sub == 2 + t, part.astype(jnp.float32), side)
        side = jnp.where(sub == 4 + t, coded(jnp.full((8, 128), part)), side)
    return table, side


def live_rows(key_ref, part_ref):
    sub8 = lax.broadcasted_iota(jnp.int32, (8, 128), 0)
    sub128 = lax.broadcasted_iota(jnp.int32, (128, 128), 0)

    def column(c, total):
        keys, parts = key_ref[c], part_ref[c]
        major = parts // 128
        minor = parts - major * 128
        lhs, rhs = [], []
        for q in range(8):
            live = (sub8 == major[q : q + 1, :]) & (keys[q : q + 1, :] >= 0)
            lhs.append(jnp.where(live, 1.0, 0.0))
            rhs.append((sub128 == minor[q : q + 1, :]).astype(jnp.float32).astype(jnp.bfloat16))
        lhs = jnp.concatenate(lhs, axis=1).astype(jnp.bfloat16)
        rhs = jnp.concatenate(rhs, axis=1)
        return total + lax.dot_general(lhs, rhs, (((1,), (1,)), ((), ())), preferred_element_type=jnp.float32)

    def columns(i, total):
        for n in range(8):
            total = column(i * 8 + n, total)
        return total

    return lax.fori_loop(0, 2, columns, jnp.zeros((8, 128), jnp.float32))


def match_rows(key_ref, part_ref, g_ref):
    sub8 = lax.broadcasted_iota(jnp.int32, (8, 128), 0)
    lane8 = lax.broadcasted_iota(jnp.int32, (8, 128), 1)
    label = (sub8 * 128 + lane8).astype(jnp.float32)
    first = lane8 < KEYS
    sub128 = lax.broadcasted_iota(jnp.int32, (128, 128), 0)
    key_at = jnp.where(sub128 >= KEYS, sub128 - KEYS, sub128)

    def column(c, total):
        keys, parts = key_ref[c], part_ref[c].astype(jnp.float32)
        pieces = pl.ds(c * 8, 8)
        count, even, odd = g_ref[pieces, 129, :], g_ref[pieces, 130, :], g_ref[pieces, 131, :]
        lhs, rhs = [], []
        for q in range(8):
            row = parts[q : q + 1, :]
            lhs.append(jnp.concatenate([jnp.where(even == row, 1.0, 0.0), jnp.where(odd == row, 1.0, 0.0)], axis=0))
            rhs.append((key_at == keys[q : q + 1, :]).astype(jnp.float32).astype(jnp.bfloat16))
        lhs = jnp.concatenate(lhs, axis=1).astype(jnp.bfloat16)
        rhs = jnp.concatenate(rhs, axis=1)
        seen = lax.dot_general(lhs, rhs, (((1,), (1,)), ((), ())), preferred_element_type=jnp.float32)
        pairs = jnp.where(first, seen[:8], seen[8:]) * count
        left = jnp.sum(jnp.where(first, pairs, 0.0), axis=1, keepdims=True)
        right = jnp.sum(jnp.where(first, 0.0, pairs), axis=1, keepdims=True)
        for r in range(8):
            total = total + jnp.where(label == even[r : r + 1, :], left[r : r + 1, :], 0.0)
            total = total + jnp.where(label == odd[r : r + 1, :], right[r : r + 1, :], 0.0)
        return total

    def columns(i, total):
        for n in range(8):
            total = column(i * 8 + n, total)
        return total

    return lax.fori_loop(0, 2, columns, jnp.zeros((8, 128), jnp.float32))


def prepare(c, key_ref, part_ref, g_ref, table, hot, column=None):
    column = c if column is None else column
    keys = key_ref[c].astype(jnp.float32)
    codes = coded(part_ref[c])
    tiles = []
    for r in range(8):
        piece = g_ref[column * 8 + r]
        high = piece.astype(jnp.bfloat16)
        low = (piece - high.astype(jnp.float32)).astype(jnp.bfloat16)
        lanes = pl.ds(r * 128, 128)
        table[0:128, lanes] = high[:128]
        table[128:256, lanes] = low[:128]
        table[256:272, lanes] = jnp.concatenate(
            [high[128:].astype(jnp.float32), low[128:].astype(jnp.float32)], axis=0
        ).astype(jnp.bfloat16)
        for t in range(2):
            tiles.append(jnp.broadcast_to(piece[132 + t : 133 + t, :], (16, 128)).astype(jnp.bfloat16))
    numbers = lax.broadcasted_iota(jnp.int32, (KEYS, 128), 0).astype(jnp.float32).astype(jnp.bfloat16)
    one, none = jnp.ones((KEYS, 128), jnp.bfloat16), jnp.zeros((KEYS, 128), jnp.bfloat16)
    for q in range(8):
        key_row = jnp.broadcast_to(keys[q : q + 1, :], (16, 128)).astype(jnp.bfloat16)
        key_hot = jnp.where(jnp.concatenate([key_row] * 4, axis=0) == numbers, one, none)
        code = jnp.broadcast_to(codes[q : q + 1, :], (16, 128)).astype(jnp.bfloat16)
        lanes = pl.ds(q % 2 * 128, 128)
        for t in range(16):
            same = jnp.where(code == tiles[t], one[:16], none[:16])
            hot[q // 2, t * KEYS : (t + 1) * KEYS, lanes] = key_hot * jnp.concatenate([same] * 4, axis=0)


def multiply(c, table, hot, joined_ref, place_ref):
    places = []
    for q2 in range(4):
        out = jnp.dot(table[...], hot[q2], preferred_element_type=jnp.float32)
        sums = out[:128] + out[128:256]
        joined_ref[c, q2 * 2] = sums[:, :128].T
        joined_ref[c, q2 * 2 + 1] = sums[:, 128:].T
        side = out[256:264] + out[264:272]
        for h in range(2):
            places.append(side[0:1, h * 128 : (h + 1) * 128])
    place_ref[c] = jnp.concatenate(places, axis=0)


def gather_kernel(
    key_hbm, part_hbm, payload_hbm, probe_key_hbm, probe_part_hbm, joined_ref, place_ref, stat_ref, g_ref,
    table_a, hot_a, table_b, hot_b, key_ref, part_ref, payload_ref, probe_key, probe_part, sums, parcels,
    loads, recv, pair_recv, send, stat_send, stat_recv,
):
    yh, z, yl, x, core = (lax.axis_index(a) for a in ALL)
    incoming = [
        pltpu.make_async_copy(src, dst, loads.at[n])
        for n, (src, dst) in enumerate(
            (
                (key_hbm, key_ref), (part_hbm, part_ref), (payload_hbm, payload_ref),
                (probe_key_hbm, probe_key), (probe_part_hbm, probe_part),
            )
        )
    ]
    for copy in incoming:
        copy.start()
    here = (x, yh * 2 + yl, z)

    def device(at, k):
        return (at[1] // 2, at[2], at[1] % 2, at[0], k)

    def slot(at, k):
        return (((at[1] % 2) * 4 + at[0]) * 2 + k) * 8 + (at[1] // 2) * 4 + at[2]

    def shifted(at, dim, delta):
        return tuple((v + delta) % 4 if d == dim else v for d, v in enumerate(at))

    def place(p, off):
        order = ORDERS[p]
        at = list(here)
        for level in range(3):
            at[order[level]] = (at[order[level]] + off[level]) % 4
        return slot(tuple(at), core)

    def block(p, index):
        return g_ref.at[index, pl.ds(CUTS[p][0], CUTS[p][1])]

    def push(p, off, level, delta):
        far = tuple((o - delta + 4) % 4 if n == level else o for n, o in enumerate(off))
        ref = block(p, place(p, off))
        pltpu.make_async_remote_copy(
            src_ref=ref, dst_ref=ref, send_sem=send.at[p], recv_sem=recv.at[p, far[0] * 16 + far[1] * 4 + far[2]],
            device_id=device(shifted(here, ORDERS[p][level], delta + 4), core), device_id_type=MESH,
        ).start()

    def pair(p, off):
        ref = block(p, place(p, off))
        pltpu.make_async_remote_copy(
            src_ref=ref, dst_ref=ref, send_sem=send.at[p], recv_sem=pair_recv.at[p],
            device_id=device(here, 1 - core), device_id_type=MESH,
        ).start()

    def arrive(p, off):
        ref = block(p, place(p, off))
        pltpu.make_async_remote_copy(
            src_ref=ref, dst_ref=ref, send_sem=send.at[p], recv_sem=recv.at[p, off[0] * 16 + off[1] * 4 + off[2]],
            device_id=device(here, 1 - core), device_id_type=MESH,
        ).wait_recv()

    barrier = pltpu.get_barrier_semaphore()
    for dim in range(3):
        for delta in (1, 2, 3):
            pl.semaphore_signal(barrier, inc=1, device_id=device(shifted(here, dim, delta), core), device_id_type=MESH)
    pl.semaphore_signal(barrier, inc=1, device_id=device(here, 1 - core), device_id_type=MESH)

    for copy in incoming[:3]:
        copy.wait()
    table, side = table_of((yh * 4 + z) * 2, key_ref, part_ref, payload_ref)
    own = slot(here, core)
    g_ref[own, :128, :] = table
    g_ref[own, 128:, :] = side
    pl.semaphore_wait(barrier, 10)

    def spread(p, off, level):
        for delta in (2, 1, -1) if level < 2 else (1, -1):
            push(p, off, level, delta)

    for level in range(3):
        for p in range(3):
            spread(p, (0, 0, 0), level)
    for p in range(3):
        pair(p, (0, 0, 0))
    for copy in incoming[3:]:
        copy.wait()
    live = live_rows(probe_key, probe_part)
    for o in (3, 1, 2):
        for p in range(3):
            arrive(p, (o, 0, 0))
            spread(p, (o, 0, 0), 1)
            spread(p, (o, 0, 0), 2)
    for p in range(3):
        for o in (3, 1, 2):
            pair(p, (o, 0, 0))

    def turn(i):
        return i + (i // 2) * (5 - 2 * i)

    def second(i, carry):
        da = turn(i)
        for p in range(3):
            for o in (3, 1):
                arrive(p, (da, o, 0))
                spread(p, (da, o, 0), 2)
                pair(p, (da, o, 0))
        return carry

    def second_far(i, carry):
        da = turn(i)
        for p in range(3):
            arrive(p, (da, 2, 0))
            spread(p, (da, 2, 0), 2)
            pair(p, (da, 2, 0))
        return carry

    def third(i, carry):
        da, db = turn(i % 4), turn(i // 4)
        delta = 1 - 2 * ((da + db) % 2)
        near = (4 - delta) % 4
        for p in range(3):
            for o in (3, 1):
                arrive(p, (da, db, o))
            push(p, (da, db, near), 2, delta)
            for o in (3, 1):
                pair(p, (da, db, o))
        return carry

    def third_far(i, carry):
        da, db = turn(i % 4), turn(i // 4)
        for p in range(3):
            arrive(p, (da, db, 2))
            pair(p, (da, db, 2))
        return carry

    lax.fori_loop(0, 4, second, 0)
    lax.fori_loop(0, 4, second_far, 0)
    lax.fori_loop(0, 16, third, 0)
    lax.fori_loop(0, 16, third_far, 0)
    for p in range(3):
        rows = pl.ds(CUTS[p][0], CUTS[p][1])
        landed = g_ref.at[pl.ds(0, 64), rows]
        pltpu.make_async_copy(landed, landed, pair_recv.at[p]).wait()

    def parcels_of(phase):
        copies = []
        for n in range(1 if phase == 0 else 3):
            target = device(here, 1 - core) if phase == 0 else device(shifted(here, phase - 1, n + 1), core)
            at = 3 * phase - 2 + n if phase else 0
            copies.append(
                pltpu.make_async_remote_copy(
                    src_ref=sums.at[phase], dst_ref=parcels.at[at], send_sem=stat_send.at[at],
                    recv_sem=stat_recv.at[at], device_id=target, device_id_type=MESH,
                )
            )
        return copies

    def begin(phase):
        for copy in parcels_of(phase):
            copy.start()

    def finish(phase):
        now = sums[phase]
        for n, copy in enumerate(parcels_of(phase)):
            copy.wait_recv()
            now = now + parcels[3 * phase - 2 + n if phase else 0]
        for copy in parcels_of(phase):
            copy.wait_send()
        return now

    sums[0] = jnp.concatenate([match_rows(probe_key, probe_part, g_ref), live], axis=0)
    begin(0)
    prepare(0, probe_key, probe_part, g_ref, table_a, hot_a)

    def joins(i, carry):
        for phase in range(1, 4):
            @pl.when(i == 2 * phase - (phase == 1))
            def _():
                sums[phase] = finish(phase - 1)
                begin(phase)

        prepare(2 * i + 1, probe_key, probe_part, g_ref, table_b, hot_b)
        multiply(2 * i, table_a, hot_a, joined_ref, place_ref)
        prepare(jnp.minimum(2 * i + 2, EARLY - 1), probe_key, probe_part, g_ref, table_a, hot_a)
        multiply(2 * i + 1, table_b, hot_b, joined_ref, place_ref)
        return carry

    lax.fori_loop(0, EARLY // 2, joins, 0)
    stat_ref[...] = finish(3)
    for p in range(3):
        rows = pl.ds(CUTS[p][0], CUTS[p][1])
        sent = g_ref.at[pl.ds(0, 127), rows]
        pltpu.make_async_copy(sent, sent, send.at[p]).wait()


def gather_and_join(build_key, build_part, build_payload, probe_key, probe_part):
    hbm = pl.BlockSpec(memory_space=pltpu.HBM)
    vmem = pl.BlockSpec(memory_space=pltpu.VMEM)
    return pl.pallas_call(
        gather_kernel,
        out_shape=(
            jax.ShapeDtypeStruct((EARLY, 8, 128, 128), jnp.float32),
            jax.ShapeDtypeStruct((EARLY, 8, 128), jnp.float32),
            jax.ShapeDtypeStruct((16, 128), jnp.float32),
            jax.ShapeDtypeStruct((128, PIECE, 128), jnp.float32),
        ),
        in_specs=[hbm] * 5,
        out_specs=(vmem, vmem, vmem, vmem),
        scratch_shapes=[
            pltpu.VMEM((272, 1024), jnp.bfloat16),
            pltpu.VMEM((4, 1024, 256), jnp.bfloat16),
            pltpu.VMEM((272, 1024), jnp.bfloat16),
            pltpu.VMEM((4, 1024, 256), jnp.bfloat16),
            pltpu.VMEM((1, 2, 128), jnp.int32),
            pltpu.SMEM((1, 2), jnp.int32),
            pltpu.VMEM((1, 2, 128, 128), jnp.float32),
            pltpu.VMEM((16, 8, 128), jnp.int32),
            pltpu.VMEM((16, 8, 128), jnp.int32),
            pltpu.VMEM((4, 16, 128), jnp.float32),
            pltpu.VMEM((10, 16, 128), jnp.float32),
            pltpu.SemaphoreType.DMA((5,)),
            pltpu.SemaphoreType.DMA((3, 64)),
            pltpu.SemaphoreType.DMA((3,)),
            pltpu.SemaphoreType.DMA((3,)),
            pltpu.SemaphoreType.DMA((10,)),
            pltpu.SemaphoreType.DMA((10,)),
        ],
        compiler_params=pltpu.CompilerParams(
            collective_id=0, has_side_effects=True, vmem_limit_bytes=20 * 1024 * 1024
        ),
        name="gather_and_join",
    )(
        *(
            pltpu.with_memory_space_constraint(a, pltpu.HBM)
            for a in (build_key, build_part, build_payload, probe_key, probe_part)
        )
    )


def finish_kernel(
    key_hbm, part_hbm, early_ref, early_place_ref, stat_ref, g_ref, joined_hbm, place_hbm, rate_hbm,
    probe_key, probe_part, joined_ref, place_ref, rate_ref, table_a, hot_a, table_b, hot_b, loads, stores,
):
    late = 16 - EARLY
    incoming = [
        pltpu.make_async_copy(src.at[pl.ds(EARLY, late)], dst, loads.at[n])
        for n, (src, dst) in enumerate(((key_hbm, probe_key), (part_hbm, probe_part)))
    ]
    for copy in incoming:
        copy.start()
    outgoing = [
        pltpu.make_async_copy(early_ref, joined_hbm.at[pl.ds(0, EARLY)], stores.at[0]),
        pltpu.make_async_copy(early_place_ref, place_hbm.at[pl.ds(0, EARLY)], stores.at[1]),
    ]
    for copy in outgoing:
        copy.start()
    rate_ref[...] = stat_ref[0:8, :] / jnp.maximum(stat_ref[8:16, :], 1.0)
    outgoing.append(pltpu.make_async_copy(rate_ref, rate_hbm, stores.at[2]))
    outgoing[-1].start()
    for copy in incoming:
        copy.wait()
    buffers = ((table_a, hot_a), (table_b, hot_b))

    def ready(n):
        prepare(n, probe_key, probe_part, g_ref, *buffers[n % 2], EARLY + n)

    ready(0)
    for n in range(late):
        if n + 1 < late:
            ready(n + 1)
        multiply(n, *buffers[n % 2], joined_ref, place_ref)
        outgoing.append(pltpu.make_async_copy(joined_ref.at[n], joined_hbm.at[EARLY + n], stores.at[3 + n]))
        outgoing[-1].start()
    outgoing.append(pltpu.make_async_copy(place_ref, place_hbm.at[pl.ds(EARLY, late)], stores.at[3 + late]))
    outgoing[-1].start()
    for copy in outgoing:
        copy.wait()


def finish_join(probe_key, probe_part, early, early_places, stats, tables):
    hbm = pl.BlockSpec(memory_space=pltpu.HBM)
    vmem = pl.BlockSpec(memory_space=pltpu.VMEM)
    late = 16 - EARLY
    return pl.pallas_call(
        finish_kernel,
        out_shape=(
            jax.ShapeDtypeStruct((16, 8, 128, 128), jnp.float32),
            jax.ShapeDtypeStruct((16, 8, 128), jnp.float32),
            jax.ShapeDtypeStruct((8, 128), jnp.float32),
        ),
        in_specs=[hbm, hbm, vmem, vmem, vmem, vmem],
        out_specs=(hbm, hbm, hbm),
        scratch_shapes=[
            pltpu.VMEM((late, 8, 128), jnp.int32),
            pltpu.VMEM((late, 8, 128), jnp.int32),
            pltpu.VMEM((late, 8, 128, 128), jnp.float32),
            pltpu.VMEM((late, 8, 128), jnp.float32),
            pltpu.VMEM((8, 128), jnp.float32),
            pltpu.VMEM((272, 1024), jnp.bfloat16),
            pltpu.VMEM((4, 1024, 256), jnp.bfloat16),
            pltpu.VMEM((272, 1024), jnp.bfloat16),
            pltpu.VMEM((4, 1024, 256), jnp.bfloat16),
            pltpu.SemaphoreType.DMA((2,)),
            pltpu.SemaphoreType.DMA((4 + late,)),
        ],
        compiler_params=pltpu.CompilerParams(vmem_limit_bytes=24 * 1024 * 1024),
        name="finish_join",
    )(
        *(pltpu.with_memory_space_constraint(a, pltpu.HBM) for a in (probe_key, probe_part)),
        early, early_places, stats, tables,
    )


def local(build_key, build_part, build_payload, probe_key, probe_part):
    probe_key, probe_part = probe_key.reshape(16, 8, 128), probe_part.reshape(16, 8, 128)
    early, early_places, stats, tables = gather_and_join(build_key, build_part, build_payload, probe_key, probe_part)
    joined, places, rate = finish_join(probe_key, probe_part, early, early_places, stats, tables)
    return (joined[None, None], places[None, None], rate.reshape(PARTS_SIZE))


def solution(mesh):
    finer = Mesh(mesh.devices.reshape(2, 4, 2, 4, 2), ALL)
    return jax.shard_map(
        local,
        mesh=finer,
        in_specs=(
            P(COL, ROW, None),
            P(COL, ROW),
            P(COL, ROW, None, None),
            P(ROW, COL, None, None, None),
            P(ROW, COL, None, None, None),
        ),
        out_specs=(P(ROW, COL, None, None, None, None), P(ROW, COL, None, None, None), P()),
        check_vma=False,
    )
```

```python
import functools

import jax
import jax.numpy as jnp
from jax import lax
from jax.experimental import pallas as pl
from jax.experimental.pallas import tpu as pltpu
from jax.sharding import Mesh
from jax.sharding import PartitionSpec as P

PARTS_SIZE = 1024
KEYS = 64
EARLY = 14
ROW = ("row_0", "row_1")
COL = ("col_0", "col_1", "col_2")
ALL = ROW + COL
MESH = pl.DeviceIdType.MESH

PIECE = 136
CUTS = ((0, 48), (48, 48), (96, 40))
ORDERS = ((0, 1, 2), (1, 2, 0), (2, 0, 1))


def coded(part):
    major = part // 128
    return (128 + part - major * 128).astype(jnp.float32) * (1 << major).astype(jnp.float32)


def table_of(tile_base, key_ref, part_ref, payload_ref):
    lane = lax.broadcasted_iota(jnp.int32, (8, 128), 1)
    sub = lax.broadcasted_iota(jnp.int32, (8, 128), 0)
    keys_col = lax.broadcasted_iota(jnp.int32, (KEYS, 128), 0)
    side_lhs = jnp.where(sub == 0, lane.astype(jnp.float32) / 2048.0, jnp.where(sub == 1, 1.0, 0.0))
    sums, sides = [], []
    for t in range(2):
        onehot = (keys_col == key_ref[0, t : t + 1, :]).astype(jnp.float32)
        sums.append(
            jnp.dot(onehot, payload_ref[0, t], precision=lax.Precision.HIGHEST, preferred_element_type=jnp.float32)
        )
        side = lax.dot_general(
            side_lhs, onehot, (((1,), (1,)), ((), ())), preferred_element_type=jnp.float32
        )
        start = (tile_base + t).astype(jnp.float32) / 16.0
        sides.append(side + jnp.where(sub[:, :KEYS] == 0, start * side[1:2, :], 0.0))
    table = jnp.concatenate(sums, axis=0).T
    side = jnp.concatenate(sides, axis=1)
    for t in range(2):
        part = part_ref[0, t]
        side = jnp.where(sub == 2 + t, part.astype(jnp.float32), side)
        side = jnp.where(sub == 4 + t, coded(jnp.full((8, 128), part)), side)
    return table, side


def live_rows(key_ref, part_ref):
    sub8 = lax.broadcasted_iota(jnp.int32, (8, 128), 0)
    sub128 = lax.broadcasted_iota(jnp.int32, (128, 128), 0)

    def column(c, total):
        keys, parts = key_ref[c], part_ref[c]
        major = parts // 128
        minor = parts - major * 128
        lhs, rhs = [], []
        for q in range(8):
            live = (sub8 == major[q : q + 1, :]) & (keys[q : q + 1, :] >= 0)
            lhs.append(jnp.where(live, 1.0, 0.0))
            rhs.append((sub128 == minor[q : q + 1, :]).astype(jnp.float32).astype(jnp.bfloat16))
        lhs = jnp.concatenate(lhs, axis=1).astype(jnp.bfloat16)
        rhs = jnp.concatenate(rhs, axis=1)
        return total + lax.dot_general(lhs, rhs, (((1,), (1,)), ((), ())), preferred_element_type=jnp.float32)

    def columns(i, total):
        for n in range(8):
            total = column(i * 8 + n, total)
        return total

    return lax.fori_loop(0, 2, columns, jnp.zeros((8, 128), jnp.float32))


def match_rows(key_ref, part_ref, g_ref):
    sub8 = lax.broadcasted_iota(jnp.int32, (8, 128), 0)
    lane8 = lax.broadcasted_iota(jnp.int32, (8, 128), 1)
    label = (sub8 * 128 + lane8).astype(jnp.float32)
    first = lane8 < KEYS
    sub128 = lax.broadcasted_iota(jnp.int32, (128, 128), 0)
    key_at = jnp.where(sub128 >= KEYS, sub128 - KEYS, sub128)

    def column(c, total):
        keys, parts = key_ref[c], part_ref[c].astype(jnp.float32)
        pieces = pl.ds(c * 8, 8)
        count, even, odd = g_ref[pieces, 129, :], g_ref[pieces, 130, :], g_ref[pieces, 131, :]
        lhs, rhs = [], []
        for q in range(8):
            row = parts[q : q + 1, :]
            lhs.append(jnp.concatenate([jnp.where(even == row, 1.0, 0.0), jnp.where(odd == row, 1.0, 0.0)], axis=0))
            rhs.append((key_at == keys[q : q + 1, :]).astype(jnp.float32).astype(jnp.bfloat16))
        lhs = jnp.concatenate(lhs, axis=1).astype(jnp.bfloat16)
        rhs = jnp.concatenate(rhs, axis=1)
        seen = lax.dot_general(lhs, rhs, (((1,), (1,)), ((), ())), preferred_element_type=jnp.float32)
        pairs = jnp.where(first, seen[:8], seen[8:]) * count
        left = jnp.sum(jnp.where(first, pairs, 0.0), axis=1, keepdims=True)
        right = jnp.sum(jnp.where(first, 0.0, pairs), axis=1, keepdims=True)
        for r in range(8):
            total = total + jnp.where(label == even[r : r + 1, :], left[r : r + 1, :], 0.0)
            total = total + jnp.where(label == odd[r : r + 1, :], right[r : r + 1, :], 0.0)
        return total

    def columns(i, total):
        for n in range(8):
            total = column(i * 8 + n, total)
        return total

    return lax.fori_loop(0, 2, columns, jnp.zeros((8, 128), jnp.float32))


def prepare(c, key_ref, part_ref, g_ref, table, hot, column=None):
    column = c if column is None else column
    keys = key_ref[c].astype(jnp.float32)
    codes = coded(part_ref[c])
    tiles = []
    for r in range(8):
        piece = g_ref[column * 8 + r]
        high = piece.astype(jnp.bfloat16)
        low = (piece - high.astype(jnp.float32)).astype(jnp.bfloat16)
        lanes = pl.ds(r * 128, 128)
        table[0:128, lanes] = high[:128]
        table[128:256, lanes] = low[:128]
        table[256:272, lanes] = jnp.concatenate(
            [high[128:].astype(jnp.float32), low[128:].astype(jnp.float32)], axis=0
        ).astype(jnp.bfloat16)
        for t in range(2):
            tiles.append(jnp.broadcast_to(piece[132 + t : 133 + t, :], (16, 128)).astype(jnp.bfloat16))
    numbers = lax.broadcasted_iota(jnp.int32, (KEYS, 128), 0).astype(jnp.float32).astype(jnp.bfloat16)
    one, none = jnp.ones((KEYS, 128), jnp.bfloat16), jnp.zeros((KEYS, 128), jnp.bfloat16)
    for q in range(8):
        key_row = jnp.broadcast_to(keys[q : q + 1, :], (16, 128)).astype(jnp.bfloat16)
        key_hot = jnp.where(jnp.concatenate([key_row] * 4, axis=0) == numbers, one, none)
        code = jnp.broadcast_to(codes[q : q + 1, :], (16, 128)).astype(jnp.bfloat16)
        lanes = pl.ds(q % 2 * 128, 128)
        for t in range(16):
            same = jnp.where(code == tiles[t], one[:16], none[:16])
            hot[q // 2, t * KEYS : (t + 1) * KEYS, lanes] = key_hot * jnp.concatenate([same] * 4, axis=0)


def multiply(c, table, hot, joined_ref, place_ref):
    places = []
    for q2 in range(4):
        out = jnp.dot(table[...], hot[q2], preferred_element_type=jnp.float32)
        sums = out[:128] + out[128:256]
        joined_ref[c, q2 * 2] = sums[:, :128].T
        joined_ref[c, q2 * 2 + 1] = sums[:, 128:].T
        side = out[256:264] + out[264:272]
        for h in range(2):
            places.append(side[0:1, h * 128 : (h + 1) * 128])
    place_ref[c] = jnp.concatenate(places, axis=0)


def gather_kernel(
    key_hbm, part_hbm, payload_hbm, probe_key_hbm, probe_part_hbm, joined_ref, place_ref, stat_ref, g_ref,
    table_a, hot_a, table_b, hot_b, key_ref, part_ref, payload_ref, probe_key, probe_part, sums, parcels,
    loads, recv, pair_recv, send, stat_send, stat_recv,
):
    yh, z, yl, x, core = (lax.axis_index(a) for a in ALL)
    incoming = [
        pltpu.make_async_copy(src, dst, loads.at[n])
        for n, (src, dst) in enumerate(
            (
                (key_hbm, key_ref), (part_hbm, part_ref), (payload_hbm, payload_ref),
                (probe_key_hbm, probe_key), (probe_part_hbm, probe_part),
            )
        )
    ]
    for copy in incoming:
        copy.start()
    here = (x, yh * 2 + yl, z)

    def device(at, k):
        return (at[1] // 2, at[2], at[1] % 2, at[0], k)

    def slot(at, k):
        return (((at[1] % 2) * 4 + at[0]) * 2 + k) * 8 + (at[1] // 2) * 4 + at[2]

    def shifted(at, dim, delta):
        return tuple((v + delta) % 4 if d == dim else v for d, v in enumerate(at))

    def place(p, off):
        order = ORDERS[p]
        at = list(here)
        for level in range(3):
            at[order[level]] = (at[order[level]] + off[level]) % 4
        return slot(tuple(at), core)

    def block(p, index):
        return g_ref.at[index, pl.ds(CUTS[p][0], CUTS[p][1])]

    def push(p, off, level, delta):
        far = tuple((o - delta + 4) % 4 if n == level else o for n, o in enumerate(off))
        ref = block(p, place(p, off))
        pltpu.make_async_remote_copy(
            src_ref=ref, dst_ref=ref, send_sem=send.at[p], recv_sem=recv.at[p, far[0] * 16 + far[1] * 4 + far[2]],
            device_id=device(shifted(here, ORDERS[p][level], delta + 4), core), device_id_type=MESH,
        ).start()

    def pair(p, off):
        ref = block(p, place(p, off))
        pltpu.make_async_remote_copy(
            src_ref=ref, dst_ref=ref, send_sem=send.at[p], recv_sem=pair_recv.at[p],
            device_id=device(here, 1 - core), device_id_type=MESH,
        ).start()

    def arrive(p, off):
        ref = block(p, place(p, off))
        pltpu.make_async_remote_copy(
            src_ref=ref, dst_ref=ref, send_sem=send.at[p], recv_sem=recv.at[p, off[0] * 16 + off[1] * 4 + off[2]],
            device_id=device(here, 1 - core), device_id_type=MESH,
        ).wait_recv()

    barrier = pltpu.get_barrier_semaphore()
    for dim in range(3):
        for delta in (1, 2, 3):
            pl.semaphore_signal(barrier, inc=1, device_id=device(shifted(here, dim, delta), core), device_id_type=MESH)
    pl.semaphore_signal(barrier, inc=1, device_id=device(here, 1 - core), device_id_type=MESH)

    for copy in incoming[:3]:
        copy.wait()
    table, side = table_of((yh * 4 + z) * 2, key_ref, part_ref, payload_ref)
    own = slot(here, core)
    g_ref[own, :128, :] = table
    g_ref[own, 128:, :] = side
    pl.semaphore_wait(barrier, 10)

    def spread(p, off, level):
        for delta in (2, 1, -1) if level < 2 else (1, -1):
            push(p, off, level, delta)

    for level in range(3):
        for p in range(3):
            spread(p, (0, 0, 0), level)
    for p in range(3):
        pair(p, (0, 0, 0))
    for copy in incoming[3:]:
        copy.wait()
    live = live_rows(probe_key, probe_part)
    for o in (3, 1, 2):
        for p in range(3):
            arrive(p, (o, 0, 0))
            spread(p, (o, 0, 0), 1)
            spread(p, (o, 0, 0), 2)
    for p in range(3):
        for o in (3, 1, 2):
            pair(p, (o, 0, 0))

    def turn(i):
        return i + (i // 2) * (5 - 2 * i)

    def second(i, carry):
        da = turn(i)
        for p in range(3):
            for o in (3, 1):
                arrive(p, (da, o, 0))
                spread(p, (da, o, 0), 2)
                pair(p, (da, o, 0))
        return carry

    def second_far(i, carry):
        da = turn(i)
        for p in range(3):
            arrive(p, (da, 2, 0))
            spread(p, (da, 2, 0), 2)
            pair(p, (da, 2, 0))
        return carry

    def third(i, carry):
        da, db = turn(i % 4), turn(i // 4)
        delta = 1 - 2 * ((da + db) % 2)
        near = (4 - delta) % 4
        for p in range(3):
            for o in (3, 1):
                arrive(p, (da, db, o))
            push(p, (da, db, near), 2, delta)
            for o in (3, 1):
                pair(p, (da, db, o))
        return carry

    def third_far(i, carry):
        da, db = turn(i % 4), turn(i // 4)
        for p in range(3):
            arrive(p, (da, db, 2))
            pair(p, (da, db, 2))
        return carry

    lax.fori_loop(0, 4, second, 0)
    lax.fori_loop(0, 4, second_far, 0)
    lax.fori_loop(0, 16, third, 0)
    lax.fori_loop(0, 16, third_far, 0)
    for p in range(3):
        rows = pl.ds(CUTS[p][0], CUTS[p][1])
        landed = g_ref.at[pl.ds(0, 64), rows]
        pltpu.make_async_copy(landed, landed, pair_recv.at[p]).wait()

    def parcels_of(phase):
        copies = []
        for n in range(1 if phase == 0 else 3):
            target = device(here, 1 - core) if phase == 0 else device(shifted(here, phase - 1, n + 1), core)
            at = 3 * phase - 2 + n if phase else 0
            copies.append(
                pltpu.make_async_remote_copy(
                    src_ref=sums.at[phase], dst_ref=parcels.at[at], send_sem=stat_send.at[at],
                    recv_sem=stat_recv.at[at], device_id=target, device_id_type=MESH,
                )
            )
        return copies

    def begin(phase):
        for copy in parcels_of(phase):
            copy.start()

    def finish(phase):
        now = sums[phase]
        for n, copy in enumerate(parcels_of(phase)):
            copy.wait_recv()
            now = now + parcels[3 * phase - 2 + n if phase else 0]
        for copy in parcels_of(phase):
            copy.wait_send()
        return now

    sums[0] = jnp.concatenate([match_rows(probe_key, probe_part, g_ref), live], axis=0)
    begin(0)
    prepare(0, probe_key, probe_part, g_ref, table_a, hot_a)

    def joins(i, carry):
        for phase in range(1, 4):
            @pl.when(i == 2 * phase - 1)
            def _():
                sums[phase] = finish(phase - 1)
                begin(phase)

        prepare(2 * i + 1, probe_key, probe_part, g_ref, table_b, hot_b)
        multiply(2 * i, table_a, hot_a, joined_ref, place_ref)
        prepare(jnp.minimum(2 * i + 2, EARLY - 1), probe_key, probe_part, g_ref, table_a, hot_a)
        multiply(2 * i + 1, table_b, hot_b, joined_ref, place_ref)
        return carry

    lax.fori_loop(0, EARLY // 2, joins, 0)
    stat_ref[...] = finish(3)
    for p in range(3):
        rows = pl.ds(CUTS[p][0], CUTS[p][1])
        sent = g_ref.at[pl.ds(0, 127), rows]
        pltpu.make_async_copy(sent, sent, send.at[p]).wait()


def gather_and_join(build_key, build_part, build_payload, probe_key, probe_part):
    hbm = pl.BlockSpec(memory_space=pltpu.HBM)
    vmem = pl.BlockSpec(memory_space=pltpu.VMEM)
    return pl.pallas_call(
        gather_kernel,
        out_shape=(
            jax.ShapeDtypeStruct((EARLY, 8, 128, 128), jnp.float32),
            jax.ShapeDtypeStruct((EARLY, 8, 128), jnp.float32),
            jax.ShapeDtypeStruct((16, 128), jnp.float32),
            jax.ShapeDtypeStruct((128, PIECE, 128), jnp.float32),
        ),
        in_specs=[hbm] * 5,
        out_specs=(vmem, vmem, vmem, vmem),
        scratch_shapes=[
            pltpu.VMEM((272, 1024), jnp.bfloat16),
            pltpu.VMEM((4, 1024, 256), jnp.bfloat16),
            pltpu.VMEM((272, 1024), jnp.bfloat16),
            pltpu.VMEM((4, 1024, 256), jnp.bfloat16),
            pltpu.VMEM((1, 2, 128), jnp.int32),
            pltpu.SMEM((1, 2), jnp.int32),
            pltpu.VMEM((1, 2, 128, 128), jnp.float32),
            pltpu.VMEM((16, 8, 128), jnp.int32),
            pltpu.VMEM((16, 8, 128), jnp.int32),
            pltpu.VMEM((4, 16, 128), jnp.float32),
            pltpu.VMEM((10, 16, 128), jnp.float32),
            pltpu.SemaphoreType.DMA((5,)),
            pltpu.SemaphoreType.DMA((3, 64)),
            pltpu.SemaphoreType.DMA((3,)),
            pltpu.SemaphoreType.DMA((3,)),
            pltpu.SemaphoreType.DMA((10,)),
            pltpu.SemaphoreType.DMA((10,)),
        ],
        compiler_params=pltpu.CompilerParams(
            collective_id=0, has_side_effects=True, vmem_limit_bytes=20 * 1024 * 1024
        ),
        name="gather_and_join",
    )(
        *(
            pltpu.with_memory_space_constraint(a, pltpu.HBM)
            for a in (build_key, build_part, build_payload, probe_key, probe_part)
        )
    )


def finish_kernel(
    key_hbm, part_hbm, early_ref, early_place_ref, stat_ref, g_ref, joined_hbm, place_hbm, rate_hbm,
    probe_key, probe_part, joined_ref, place_ref, rate_ref, table_a, hot_a, table_b, hot_b, loads, stores,
):
    late = 16 - EARLY
    incoming = [
        pltpu.make_async_copy(src.at[pl.ds(EARLY, late)], dst, loads.at[n])
        for n, (src, dst) in enumerate(((key_hbm, probe_key), (part_hbm, probe_part)))
    ]
    for copy in incoming:
        copy.start()
    outgoing = [
        pltpu.make_async_copy(early_ref, joined_hbm.at[pl.ds(0, EARLY)], stores.at[0]),
        pltpu.make_async_copy(early_place_ref, place_hbm.at[pl.ds(0, EARLY)], stores.at[1]),
    ]
    for copy in outgoing:
        copy.start()
    rate_ref[...] = stat_ref[0:8, :] / jnp.maximum(stat_ref[8:16, :], 1.0)
    outgoing.append(pltpu.make_async_copy(rate_ref, rate_hbm, stores.at[2]))
    outgoing[-1].start()
    for copy in incoming:
        copy.wait()
    buffers = ((table_a, hot_a), (table_b, hot_b))

    def ready(n):
        prepare(n, probe_key, probe_part, g_ref, *buffers[n % 2], EARLY + n)

    ready(0)
    for n in range(late):
        if n + 1 < late:
            ready(n + 1)
        multiply(n, *buffers[n % 2], joined_ref, place_ref)
        outgoing.append(pltpu.make_async_copy(joined_ref.at[n], joined_hbm.at[EARLY + n], stores.at[3 + n]))
        outgoing[-1].start()
    outgoing.append(pltpu.make_async_copy(place_ref, place_hbm.at[pl.ds(EARLY, late)], stores.at[3 + late]))
    outgoing[-1].start()
    for copy in outgoing:
        copy.wait()


def finish_join(probe_key, probe_part, early, early_places, stats, tables):
    hbm = pl.BlockSpec(memory_space=pltpu.HBM)
    vmem = pl.BlockSpec(memory_space=pltpu.VMEM)
    late = 16 - EARLY
    return pl.pallas_call(
        finish_kernel,
        out_shape=(
            jax.ShapeDtypeStruct((16, 8, 128, 128), jnp.float32),
            jax.ShapeDtypeStruct((16, 8, 128), jnp.float32),
            jax.ShapeDtypeStruct((8, 128), jnp.float32),
        ),
        in_specs=[hbm, hbm, vmem, vmem, vmem, vmem],
        out_specs=(hbm, hbm, hbm),
        scratch_shapes=[
            pltpu.VMEM((late, 8, 128), jnp.int32),
            pltpu.VMEM((late, 8, 128), jnp.int32),
            pltpu.VMEM((late, 8, 128, 128), jnp.float32),
            pltpu.VMEM((late, 8, 128), jnp.float32),
            pltpu.VMEM((8, 128), jnp.float32),
            pltpu.VMEM((272, 1024), jnp.bfloat16),
            pltpu.VMEM((4, 1024, 256), jnp.bfloat16),
            pltpu.VMEM((272, 1024), jnp.bfloat16),
            pltpu.VMEM((4, 1024, 256), jnp.bfloat16),
            pltpu.SemaphoreType.DMA((2,)),
            pltpu.SemaphoreType.DMA((4 + late,)),
        ],
        compiler_params=pltpu.CompilerParams(vmem_limit_bytes=24 * 1024 * 1024),
        name="finish_join",
    )(
        *(pltpu.with_memory_space_constraint(a, pltpu.HBM) for a in (probe_key, probe_part)),
        early, early_places, stats, tables,
    )


def local(build_key, build_part, build_payload, probe_key, probe_part):
    probe_key, probe_part = probe_key.reshape(16, 8, 128), probe_part.reshape(16, 8, 128)
    early, early_places, stats, tables = gather_and_join(build_key, build_part, build_payload, probe_key, probe_part)
    joined, places, rate = finish_join(probe_key, probe_part, early, early_places, stats, tables)
    return (joined[None, None], places[None, None], rate.reshape(PARTS_SIZE))


def solution(mesh):
    finer = Mesh(mesh.devices.reshape(2, 4, 2, 4, 2), ALL)
    return jax.shard_map(
        local,
        mesh=finer,
        in_specs=(
            P(COL, ROW, None),
            P(COL, ROW),
            P(COL, ROW, None, None),
            P(ROW, COL, None, None, None),
            P(ROW, COL, None, None, None),
        ),
        out_specs=(P(ROW, COL, None, None, None, None), P(ROW, COL, None, None, None), P()),
        check_vma=False,
    )
```

```python
import functools

import jax
import jax.numpy as jnp
from jax import lax
from jax.experimental import pallas as pl
from jax.experimental.pallas import tpu as pltpu
from jax.sharding import Mesh
from jax.sharding import PartitionSpec as P

PARTS_SIZE = 1024
KEYS = 64
EARLY = 14
ROW = ("row_0", "row_1")
COL = ("col_0", "col_1", "col_2")
ALL = ROW + COL
MESH = pl.DeviceIdType.MESH

PIECE = 136
CUTS = ((0, 48), (48, 48), (96, 40))
ORDERS = ((0, 1, 2), (1, 2, 0), (2, 0, 1))


def coded(part):
    major = part // 128
    return (128 + part - major * 128).astype(jnp.float32) * (1 << major).astype(jnp.float32)


def table_of(tile_base, key_ref, part_ref, payload_ref):
    lane = lax.broadcasted_iota(jnp.int32, (8, 128), 1)
    sub = lax.broadcasted_iota(jnp.int32, (8, 128), 0)
    keys_col = lax.broadcasted_iota(jnp.int32, (KEYS, 128), 0)
    side_lhs = jnp.where(sub == 0, lane.astype(jnp.float32) / 2048.0, jnp.where(sub == 1, 1.0, 0.0))
    sums, sides = [], []
    for t in range(2):
        onehot = (keys_col == key_ref[0, t : t + 1, :]).astype(jnp.float32)
        sums.append(
            jnp.dot(onehot, payload_ref[0, t], precision=lax.Precision.HIGHEST, preferred_element_type=jnp.float32)
        )
        side = lax.dot_general(
            side_lhs, onehot, (((1,), (1,)), ((), ())), preferred_element_type=jnp.float32
        )
        start = (tile_base + t).astype(jnp.float32) / 16.0
        sides.append(side + jnp.where(sub[:, :KEYS] == 0, start * side[1:2, :], 0.0))
    table = jnp.concatenate(sums, axis=0).T
    side = jnp.concatenate(sides, axis=1)
    for t in range(2):
        part = part_ref[0, t]
        side = jnp.where(sub == 2 + t, part.astype(jnp.float32), side)
        side = jnp.where(sub == 4 + t, coded(jnp.full((8, 128), part)), side)
    return table, side


def live_rows(key_ref, part_ref):
    sub8 = lax.broadcasted_iota(jnp.int32, (8, 128), 0)
    sub128 = lax.broadcasted_iota(jnp.int32, (128, 128), 0)

    def column(c, total):
        keys, parts = key_ref[c], part_ref[c]
        major = parts // 128
        minor = parts - major * 128
        lhs, rhs = [], []
        for q in range(8):
            live = (sub8 == major[q : q + 1, :]) & (keys[q : q + 1, :] >= 0)
            lhs.append(jnp.where(live, 1.0, 0.0))
            rhs.append((sub128 == minor[q : q + 1, :]).astype(jnp.float32).astype(jnp.bfloat16))
        lhs = jnp.concatenate(lhs, axis=1).astype(jnp.bfloat16)
        rhs = jnp.concatenate(rhs, axis=1)
        return total + lax.dot_general(lhs, rhs, (((1,), (1,)), ((), ())), preferred_element_type=jnp.float32)

    def columns(i, total):
        for n in range(8):
            total = column(i * 8 + n, total)
        return total

    return lax.fori_loop(0, 2, columns, jnp.zeros((8, 128), jnp.float32))


def match_rows(key_ref, part_ref, g_ref):
    sub8 = lax.broadcasted_iota(jnp.int32, (8, 128), 0)
    lane8 = lax.broadcasted_iota(jnp.int32, (8, 128), 1)
    label = (sub8 * 128 + lane8).astype(jnp.float32)
    first = lane8 < KEYS
    sub128 = lax.broadcasted_iota(jnp.int32, (128, 128), 0)
    key_at = jnp.where(sub128 >= KEYS, sub128 - KEYS, sub128)

    def column(c, total):
        keys, parts = key_ref[c], part_ref[c].astype(jnp.float32)
        pieces = pl.ds(c * 8, 8)
        count, even, odd = g_ref[pieces, 129, :], g_ref[pieces, 130, :], g_ref[pieces, 131, :]
        lhs, rhs = [], []
        for q in range(8):
            row = parts[q : q + 1, :]
            lhs.append(jnp.concatenate([jnp.where(even == row, 1.0, 0.0), jnp.where(odd == row, 1.0, 0.0)], axis=0))
            rhs.append((key_at == keys[q : q + 1, :]).astype(jnp.float32).astype(jnp.bfloat16))
        lhs = jnp.concatenate(lhs, axis=1).astype(jnp.bfloat16)
        rhs = jnp.concatenate(rhs, axis=1)
        seen = lax.dot_general(lhs, rhs, (((1,), (1,)), ((), ())), preferred_element_type=jnp.float32)
        pairs = jnp.where(first, seen[:8], seen[8:]) * count
        left = jnp.sum(jnp.where(first, pairs, 0.0), axis=1, keepdims=True)
        right = jnp.sum(jnp.where(first, 0.0, pairs), axis=1, keepdims=True)
        for r in range(8):
            total = total + jnp.where(label == even[r : r + 1, :], left[r : r + 1, :], 0.0)
            total = total + jnp.where(label == odd[r : r + 1, :], right[r : r + 1, :], 0.0)
        return total

    def columns(i, total):
        for n in range(8):
            total = column(i * 8 + n, total)
        return total

    return lax.fori_loop(0, 2, columns, jnp.zeros((8, 128), jnp.float32))


def prepare(c, key_ref, part_ref, g_ref, table, hot, column=None):
    column = c if column is None else column
    keys = key_ref[c].astype(jnp.float32)
    codes = coded(part_ref[c])
    tiles = []
    for r in range(8):
        piece = g_ref[column * 8 + r]
        high = piece.astype(jnp.bfloat16)
        low = (piece - high.astype(jnp.float32)).astype(jnp.bfloat16)
        lanes = pl.ds(r * 128, 128)
        table[0:128, lanes] = high[:128]
        table[128:256, lanes] = low[:128]
        table[256:272, lanes] = jnp.concatenate(
            [high[128:].astype(jnp.float32), low[128:].astype(jnp.float32)], axis=0
        ).astype(jnp.bfloat16)
        for t in range(2):
            tiles.append(jnp.broadcast_to(piece[132 + t : 133 + t, :], (16, 128)).astype(jnp.bfloat16))
    numbers = lax.broadcasted_iota(jnp.int32, (KEYS, 128), 0).astype(jnp.float32).astype(jnp.bfloat16)
    one, none = jnp.ones((KEYS, 128), jnp.bfloat16), jnp.zeros((KEYS, 128), jnp.bfloat16)
    for q in range(8):
        key_row = jnp.broadcast_to(keys[q : q + 1, :], (16, 128)).astype(jnp.bfloat16)
        key_hot = jnp.where(jnp.concatenate([key_row] * 4, axis=0) == numbers, one, none)
        code = jnp.broadcast_to(codes[q : q + 1, :], (16, 128)).astype(jnp.bfloat16)
        lanes = pl.ds(q % 2 * 128, 128)
        for t in range(16):
            same = jnp.where(code == tiles[t], one[:16], none[:16])
            hot[q // 2, t * KEYS : (t + 1) * KEYS, lanes] = key_hot * jnp.concatenate([same] * 4, axis=0)


def multiply(c, table, hot, joined_ref, place_ref):
    places = []
    for q2 in range(4):
        out = jnp.dot(table[...], hot[q2], preferred_element_type=jnp.float32)
        sums = out[:128] + out[128:256]
        joined_ref[c, q2 * 2] = sums[:, :128].T
        joined_ref[c, q2 * 2 + 1] = sums[:, 128:].T
        side = out[256:264] + out[264:272]
        for h in range(2):
            places.append(side[0:1, h * 128 : (h + 1) * 128])
    place_ref[c] = jnp.concatenate(places, axis=0)


def gather_kernel(
    key_hbm, part_hbm, payload_hbm, probe_key_hbm, probe_part_hbm, joined_ref, place_ref, stat_ref, g_ref,
    table_a, hot_a, table_b, hot_b, key_ref, part_ref, payload_ref, probe_key, probe_part, sums, parcels,
    loads, recv, pair_recv, send, stat_send, stat_recv,
):
    yh, z, yl, x, core = (lax.axis_index(a) for a in ALL)
    incoming = [
        pltpu.make_async_copy(src, dst, loads.at[n])
        for n, (src, dst) in enumerate(
            (
                (key_hbm, key_ref), (part_hbm, part_ref), (payload_hbm, payload_ref),
                (probe_key_hbm, probe_key), (probe_part_hbm, probe_part),
            )
        )
    ]
    for copy in incoming:
        copy.start()
    here = (x, yh * 2 + yl, z)

    def device(at, k):
        return (at[1] // 2, at[2], at[1] % 2, at[0], k)

    def slot(at, k):
        return (((at[1] % 2) * 4 + at[0]) * 2 + k) * 8 + (at[1] // 2) * 4 + at[2]

    def shifted(at, dim, delta):
        return tuple((v + delta) % 4 if d == dim else v for d, v in enumerate(at))

    def place(p, off):
        order = ORDERS[p]
        at = list(here)
        for level in range(3):
            at[order[level]] = (at[order[level]] + off[level]) % 4
        return slot(tuple(at), core)

    def block(p, index):
        return g_ref.at[index, pl.ds(CUTS[p][0], CUTS[p][1])]

    def push(p, off, level, delta):
        far = tuple((o - delta + 4) % 4 if n == level else o for n, o in enumerate(off))
        ref = block(p, place(p, off))
        pltpu.make_async_remote_copy(
            src_ref=ref, dst_ref=ref, send_sem=send.at[p], recv_sem=recv.at[p, far[0] * 16 + far[1] * 4 + far[2]],
            device_id=device(shifted(here, ORDERS[p][level], delta + 4), core), device_id_type=MESH,
        ).start()

    def pair(p, off):
        ref = block(p, place(p, off))
        pltpu.make_async_remote_copy(
            src_ref=ref, dst_ref=ref, send_sem=send.at[p], recv_sem=pair_recv.at[p],
            device_id=device(here, 1 - core), device_id_type=MESH,
        ).start()

    def arrive(p, off):
        ref = block(p, place(p, off))
        pltpu.make_async_remote_copy(
            src_ref=ref, dst_ref=ref, send_sem=send.at[p], recv_sem=recv.at[p, off[0] * 16 + off[1] * 4 + off[2]],
            device_id=device(here, 1 - core), device_id_type=MESH,
        ).wait_recv()

    barrier = pltpu.get_barrier_semaphore()
    for dim in range(3):
        for delta in (1, 2, 3):
            pl.semaphore_signal(barrier, inc=1, device_id=device(shifted(here, dim, delta), core), device_id_type=MESH)
    pl.semaphore_signal(barrier, inc=1, device_id=device(here, 1 - core), device_id_type=MESH)

    for copy in incoming[:3]:
        copy.wait()
    table, side = table_of((yh * 4 + z) * 2, key_ref, part_ref, payload_ref)
    own = slot(here, core)
    g_ref[own, :128, :] = table
    g_ref[own, 128:, :] = side
    pl.semaphore_wait(barrier, 10)

    def spread(p, off, level):
        for delta in (2, 1, -1) if level < 2 else (1, -1):
            push(p, off, level, delta)

    for level in range(3):
        for p in range(3):
            spread(p, (0, 0, 0), level)
    for p in range(3):
        pair(p, (0, 0, 0))
    for copy in incoming[3:]:
        copy.wait()
    live = live_rows(probe_key, probe_part)
    for o in (3, 1, 2):
        for p in range(3):
            arrive(p, (o, 0, 0))
            spread(p, (o, 0, 0), 1)
            spread(p, (o, 0, 0), 2)
    for p in range(3):
        for o in (3, 1, 2):
            pair(p, (o, 0, 0))

    def turn(i):
        return i + (i // 2) * (5 - 2 * i)

    def second(i, carry):
        da = turn(i)
        for p in range(3):
            for o in (3, 1):
                arrive(p, (da, o, 0))
                spread(p, (da, o, 0), 2)
                pair(p, (da, o, 0))
        return carry

    def second_far(i, carry):
        da = turn(i)
        for p in range(3):
            arrive(p, (da, 2, 0))
            spread(p, (da, 2, 0), 2)
            pair(p, (da, 2, 0))
        return carry

    def third(i, carry):
        da, db = turn(i % 4), turn(i // 4)
        delta = 1 - 2 * ((da + db) % 2)
        near = (4 - delta) % 4
        for p in range(3):
            arrive(p, (da, db, near))
            push(p, (da, db, near), 2, delta)
        for p in range(3):
            arrive(p, (da, db, 4 - near))
            for o in (near, 4 - near):
                pair(p, (da, db, o))
        return carry

    def third_far(i, carry):
        da, db = turn(i % 4), turn(i // 4)
        for p in range(3):
            arrive(p, (da, db, 2))
            pair(p, (da, db, 2))
        return carry

    lax.fori_loop(0, 4, second, 0)
    lax.fori_loop(0, 4, second_far, 0)
    lax.fori_loop(0, 16, third, 0)
    lax.fori_loop(0, 16, third_far, 0)
    for p in range(3):
        rows = pl.ds(CUTS[p][0], CUTS[p][1])
        landed = g_ref.at[pl.ds(0, 64), rows]
        pltpu.make_async_copy(landed, landed, pair_recv.at[p]).wait()

    def parcels_of(phase):
        copies = []
        for n in range(1 if phase == 0 else 3):
            target = device(here, 1 - core) if phase == 0 else device(shifted(here, phase - 1, n + 1), core)
            at = 3 * phase - 2 + n if phase else 0
            copies.append(
                pltpu.make_async_remote_copy(
                    src_ref=sums.at[phase], dst_ref=parcels.at[at], send_sem=stat_send.at[at],
                    recv_sem=stat_recv.at[at], device_id=target, device_id_type=MESH,
                )
            )
        return copies

    def begin(phase):
        for copy in parcels_of(phase):
            copy.start()

    def finish(phase):
        now = sums[phase]
        for n, copy in enumerate(parcels_of(phase)):
            copy.wait_recv()
            now = now + parcels[3 * phase - 2 + n if phase else 0]
        for copy in parcels_of(phase):
            copy.wait_send()
        return now

    sums[0] = jnp.concatenate([match_rows(probe_key, probe_part, g_ref), live], axis=0)
    begin(0)
    prepare(0, probe_key, probe_part, g_ref, table_a, hot_a)

    def joins(i, carry):
        for phase in range(1, 4):
            @pl.when(i == 2 * phase - 1)
            def _():
                sums[phase] = finish(phase - 1)
                begin(phase)

        prepare(2 * i + 1, probe_key, probe_part, g_ref, table_b, hot_b)
        multiply(2 * i, table_a, hot_a, joined_ref, place_ref)
        prepare(jnp.minimum(2 * i + 2, EARLY - 1), probe_key, probe_part, g_ref, table_a, hot_a)
        multiply(2 * i + 1, table_b, hot_b, joined_ref, place_ref)
        return carry

    lax.fori_loop(0, EARLY // 2, joins, 0)
    stat_ref[...] = finish(3)
    for p in range(3):
        rows = pl.ds(CUTS[p][0], CUTS[p][1])
        sent = g_ref.at[pl.ds(0, 127), rows]
        pltpu.make_async_copy(sent, sent, send.at[p]).wait()


def gather_and_join(build_key, build_part, build_payload, probe_key, probe_part):
    hbm = pl.BlockSpec(memory_space=pltpu.HBM)
    vmem = pl.BlockSpec(memory_space=pltpu.VMEM)
    return pl.pallas_call(
        gather_kernel,
        out_shape=(
            jax.ShapeDtypeStruct((EARLY, 8, 128, 128), jnp.float32),
            jax.ShapeDtypeStruct((EARLY, 8, 128), jnp.float32),
            jax.ShapeDtypeStruct((16, 128), jnp.float32),
            jax.ShapeDtypeStruct((128, PIECE, 128), jnp.float32),
        ),
        in_specs=[hbm] * 5,
        out_specs=(vmem, vmem, vmem, vmem),
        scratch_shapes=[
            pltpu.VMEM((272, 1024), jnp.bfloat16),
            pltpu.VMEM((4, 1024, 256), jnp.bfloat16),
            pltpu.VMEM((272, 1024), jnp.bfloat16),
            pltpu.VMEM((4, 1024, 256), jnp.bfloat16),
            pltpu.VMEM((1, 2, 128), jnp.int32),
            pltpu.SMEM((1, 2), jnp.int32),
            pltpu.VMEM((1, 2, 128, 128), jnp.float32),
            pltpu.VMEM((16, 8, 128), jnp.int32),
            pltpu.VMEM((16, 8, 128), jnp.int32),
            pltpu.VMEM((4, 16, 128), jnp.float32),
            pltpu.VMEM((10, 16, 128), jnp.float32),
            pltpu.SemaphoreType.DMA((5,)),
            pltpu.SemaphoreType.DMA((3, 64)),
            pltpu.SemaphoreType.DMA((3,)),
            pltpu.SemaphoreType.DMA((3,)),
            pltpu.SemaphoreType.DMA((10,)),
            pltpu.SemaphoreType.DMA((10,)),
        ],
        compiler_params=pltpu.CompilerParams(
            collective_id=0, has_side_effects=True, vmem_limit_bytes=20 * 1024 * 1024
        ),
        name="gather_and_join",
    )(
        *(
            pltpu.with_memory_space_constraint(a, pltpu.HBM)
            for a in (build_key, build_part, build_payload, probe_key, probe_part)
        )
    )


def finish_kernel(
    key_hbm, part_hbm, early_ref, early_place_ref, stat_ref, g_ref, joined_hbm, place_hbm, rate_hbm,
    probe_key, probe_part, joined_ref, place_ref, rate_ref, table_a, hot_a, table_b, hot_b, loads, stores,
):
    late = 16 - EARLY
    incoming = [
        pltpu.make_async_copy(src.at[pl.ds(EARLY, late)], dst, loads.at[n])
        for n, (src, dst) in enumerate(((key_hbm, probe_key), (part_hbm, probe_part)))
    ]
    for copy in incoming:
        copy.start()
    outgoing = [
        pltpu.make_async_copy(early_ref, joined_hbm.at[pl.ds(0, EARLY)], stores.at[0]),
        pltpu.make_async_copy(early_place_ref, place_hbm.at[pl.ds(0, EARLY)], stores.at[1]),
    ]
    for copy in outgoing:
        copy.start()
    rate_ref[...] = stat_ref[0:8, :] / jnp.maximum(stat_ref[8:16, :], 1.0)
    outgoing.append(pltpu.make_async_copy(rate_ref, rate_hbm, stores.at[2]))
    outgoing[-1].start()
    for copy in incoming:
        copy.wait()
    buffers = ((table_a, hot_a), (table_b, hot_b))

    def ready(n):
        prepare(n, probe_key, probe_part, g_ref, *buffers[n % 2], EARLY + n)

    ready(0)
    for n in range(late):
        if n + 1 < late:
            ready(n + 1)
        multiply(n, *buffers[n % 2], joined_ref, place_ref)
        outgoing.append(pltpu.make_async_copy(joined_ref.at[n], joined_hbm.at[EARLY + n], stores.at[3 + n]))
        outgoing[-1].start()
    outgoing.append(pltpu.make_async_copy(place_ref, place_hbm.at[pl.ds(EARLY, late)], stores.at[3 + late]))
    outgoing[-1].start()
    for copy in outgoing:
        copy.wait()


def finish_join(probe_key, probe_part, early, early_places, stats, tables):
    hbm = pl.BlockSpec(memory_space=pltpu.HBM)
    vmem = pl.BlockSpec(memory_space=pltpu.VMEM)
    late = 16 - EARLY
    return pl.pallas_call(
        finish_kernel,
        out_shape=(
            jax.ShapeDtypeStruct((16, 8, 128, 128), jnp.float32),
            jax.ShapeDtypeStruct((16, 8, 128), jnp.float32),
            jax.ShapeDtypeStruct((8, 128), jnp.float32),
        ),
        in_specs=[hbm, hbm, vmem, vmem, vmem, vmem],
        out_specs=(hbm, hbm, hbm),
        scratch_shapes=[
            pltpu.VMEM((late, 8, 128), jnp.int32),
            pltpu.VMEM((late, 8, 128), jnp.int32),
            pltpu.VMEM((late, 8, 128, 128), jnp.float32),
            pltpu.VMEM((late, 8, 128), jnp.float32),
            pltpu.VMEM((8, 128), jnp.float32),
            pltpu.VMEM((272, 1024), jnp.bfloat16),
            pltpu.VMEM((4, 1024, 256), jnp.bfloat16),
            pltpu.VMEM((272, 1024), jnp.bfloat16),
            pltpu.VMEM((4, 1024, 256), jnp.bfloat16),
            pltpu.SemaphoreType.DMA((2,)),
            pltpu.SemaphoreType.DMA((4 + late,)),
        ],
        compiler_params=pltpu.CompilerParams(vmem_limit_bytes=24 * 1024 * 1024),
        name="finish_join",
    )(
        *(pltpu.with_memory_space_constraint(a, pltpu.HBM) for a in (probe_key, probe_part)),
        early, early_places, stats, tables,
    )


def local(build_key, build_part, build_payload, probe_key, probe_part):
    probe_key, probe_part = probe_key.reshape(16, 8, 128), probe_part.reshape(16, 8, 128)
    early, early_places, stats, tables = gather_and_join(build_key, build_part, build_payload, probe_key, probe_part)
    joined, places, rate = finish_join(probe_key, probe_part, early, early_places, stats, tables)
    return (joined[None, None], places[None, None], rate.reshape(PARTS_SIZE))


def solution(mesh):
    finer = Mesh(mesh.devices.reshape(2, 4, 2, 4, 2), ALL)
    return jax.shard_map(
        local,
        mesh=finer,
        in_specs=(
            P(COL, ROW, None),
            P(COL, ROW),
            P(COL, ROW, None, None),
            P(ROW, COL, None, None, None),
            P(ROW, COL, None, None, None),
        ),
        out_specs=(P(ROW, COL, None, None, None, None), P(ROW, COL, None, None, None), P()),
        check_vma=False,
    )
```
